512 devices in a mesh: tm: 8 (over x, core), lat: 16 (over y, z_hi), lon: 4 (over z_lo).
Axes of the slice: x: 4, y: 8, z: 8 (z_hi: 2, z_lo: 4; z = z_hi * 4 + z_lo), core: 2. Of those that a mesh axis runs over, the one named last changes fastest.
Arguments:
- control: float32 [16, 8, 256, 512], P(None, None, 'lat', 'lon'), may hold values from -6 to 6
- ens_pert: bfloat16 [8, 16, 8, 256, 512], P('tm', None, None, 'lat', 'lon'), may hold values from -6 to 6
- lat_filter: bfloat16 [256, 256], replicated, may hold values from 0 to 2.5, as said below
- lon_filter: bfloat16 [512, 512], replicated, may hold values from 0 to 2.5, as said below
- interp_lat: float32 [512, 18], P('lat'), may hold values from -1.5 to 1.5
- interp_lon: float32 [1024, 130], P('lon'), may hold values from -0.5 to 0.5
- obs_cell: int32 [8, 8, 16, 4, 64], P('tm', None, 'lat', 'lon'), may hold values from 0 to 65535
- obs_count: int32 [8, 8, 16, 4], P('tm', None, 'lat', 'lon'), may hold values from 1 to 64, as said below
- obs_value: float32 [8, 8, 16, 4, 64], P('tm', None, 'lat', 'lon'), may hold values from -18 to 18
- obs_weight: float32 [8, 8, 16, 4, 64], P('tm', None, 'lat', 'lon'), may hold values from 0.1 to 0.4
Outputs:
- gradient: float32 [16, 8, 256, 512], P(None, None, 'lat', 'lon')
The draws below stay inside these ranges and needn't reach their ends.
Inputs may be any that keep to these rules, and one draw needn't show every extreme that they name: `lat_filter`: within the latitude spreading matrix all entries are non-negative. `lon_filter`: entries are non-negative. `obs_count`: each count is at least 1 and at most 64; in every draw some count equals 64.
All inputs are finite; a program needn't handle non-finite values.
Results may differ from the reference program's by a relative error of at most 0.0003.
Values sent between devices are 32-bit elements; how exact they have to be, the bound alone decides.
A program may use at most 64 MiB of HBM per device.

```python
import math
import jax
import jax.numpy as jnp
from jax import lax

MEM = 16
LEV = 8
CLAT = 16
CLON = 128
CAP = 64
SLOTS = 8
NLAT = 256
NLON = 512
FLAT = 32
FLON = 256
N_TM = 8
N_LAT = 16
N_LON = 4


def filter_table(key, length, reach, periodic):
    places = jnp.arange(length)
    distance = jnp.abs(places[:, None] - places[None, :]).astype(jnp.float32)
    if periodic:
        distance = jnp.minimum(distance, length - distance)
    factor = jax.random.uniform(key, (length, length), jnp.float32, 0.5, 1.5)
    table = jnp.exp(-distance / reach) * factor / jnp.sqrt(jnp.float32(reach))
    table = table + 0.5 * jnp.eye(length, dtype=jnp.float32)
    return table.astype(jnp.bfloat16)


def draw_lat_filter(key, part):
    return filter_table(jax.random.fold_in(key, 11), NLAT, 2.0 * CLAT, False)


def draw_lon_filter(key, part):
    return filter_table(jax.random.fold_in(key, 23), NLON, 2.0 * CLON, True)


def draw_obs_count(key, part):
    first, second, third = jax.random.split(jax.random.fold_in(key, 37), 3)
    shape = (N_TM, SLOTS, N_LAT, N_LON)
    level = jax.random.randint(first, (1, SLOTS, 1, 1), 1, 5)
    upper = 1 + CAP * level // 4
    counts = jax.random.randint(second, shape, 1, upper + 1)
    counts = jnp.minimum(counts, CAP)
    choose = jax.random.randint(third, (), 0, N_TM * SLOTS * N_LAT * N_LON)
    counts = counts.reshape(-1).at[choose].set(CAP).reshape(shape)
    return counts.astype(jnp.int32)


def with_ends(entries, own_key, smallest, high):
    longest = entries.shape.index(max(entries.shape))
    spots = []
    for shift in (0, 1):
        where = [jax.random.randint(jax.random.fold_in(own_key, axis), (), 0, length) for axis, length in enumerate(entries.shape)]
        where[longest] = (where[longest] + shift) % entries.shape[longest]
        spots.append(tuple(where))
    return entries.at[spots[0]].set(smallest).at[spots[1]].set(high)


def level_of(key, dims, cuts, smallest, high):
    def one(position, parts):
        steps = jax.random.uniform(jax.random.fold_in(jax.random.fold_in(key, 6), position), (parts,), jnp.float32, smallest / len(cuts), high / len(cuts))
        return jnp.repeat(jnp.exp(steps), dims[position] // parts).reshape((-1,) + (1,) * (len(dims) - position - 1))

    loudness = one(*cuts[0])
    for cut in cuts[1:]:
        loudness = loudness * one(*cut)
    return loudness


def bell_draw(rng, shape, width, most, cuts=(), kind=jnp.bfloat16):
    drawn = jax.random.normal(rng, shape, jnp.float32) * width
    if len(cuts) > 0:
        drawn = level_of(rng, shape, cuts, -0.22, 0.18) * drawn
    return jnp.clip(drawn, min=-most, max=most).astype(kind)


def setup_inputs(seed: int = 0) -> dict:
    streams_of = jax.random.split(jax.random.key(seed), 11)
    return {
        "control": bell_draw(streams_of[0], (MEM, LEV, NLAT, NLON), 1.0, 6.0, ((2, 16), (3, 4)), jnp.float32),
        "ens_pert": bell_draw(streams_of[1], (SLOTS, MEM, LEV, NLAT, NLON), 1.0, 6.0, ((0, 8), (3, 16), (4, 4))),
        "lat_filter": draw_lat_filter(jax.random.fold_in(streams_of[10], 71), 0),
        "lon_filter": draw_lon_filter(jax.random.fold_in(streams_of[10], 71), 0),
        "interp_lat": bell_draw(streams_of[4], (N_LAT * FLAT, CLAT + 2), (CLAT + 2) ** -0.5, 1.5, ((0, 16),), jnp.float32),
        "interp_lon": bell_draw(streams_of[5], (N_LON * FLON, CLON + 2), (CLON + 2) ** -0.5, 0.5, ((0, 4),), jnp.float32),
        "obs_cell": with_ends(jax.random.randint(streams_of[6], (N_TM, SLOTS, N_LAT, N_LON, CAP), 0, LEV * FLAT * FLON), jax.random.fold_in(streams_of[6], 1), 0, (LEV * FLAT * FLON) - 1).astype(jnp.int32),
        "obs_count": draw_obs_count(jax.random.fold_in(streams_of[10], 71), 0),
        "obs_value": bell_draw(streams_of[8], (N_TM, SLOTS, N_LAT, N_LON, CAP), 3.0, 18.0, ((0, 8), (2, 16), (3, 4)), jnp.float32),
        "obs_weight": jnp.clip(jnp.exp(math.log(0.4) - 1.3862944 * jax.random.uniform(streams_of[9], (N_TM, SLOTS, N_LAT, N_LON, CAP), jnp.float32) ** level_of(streams_of[9], (N_TM, SLOTS, N_LAT, N_LON, CAP), ((0, 8), (2, 16), (3, 4)), -0.2, 0.2)), 0.1, 0.4),
    }


HIGHEST = lax.Precision.HIGHEST

def spread_both(source, lat_matrix, lon_matrix):
    across = jnp.einsum('ab,mlbc->mlac', lat_matrix, source, precision=HIGHEST)
    return jnp.einsum('mlac,dc->mlad', across, lon_matrix, precision=HIGHEST)

def to_fine(increment, interp_lat, interp_lon):
    padded = jnp.pad(increment, ((0, 0), (1, 1), (0, 0)))
    padded = jnp.concatenate([padded[:, :, -1:], padded, padded[:, :, :1]], axis=2)
    lat_index = (jnp.arange(N_LAT)[:, None] * CLAT + jnp.arange(CLAT + 2)[None, :]).astype(jnp.int32)
    lon_index = (jnp.arange(N_LON)[:, None] * CLON + jnp.arange(CLON + 2)[None, :]).astype(jnp.int32)
    windows = padded[:, lat_index][:, :, :, lon_index]
    lat_blocks = interp_lat.reshape(N_LAT, FLAT, CLAT + 2)
    lon_blocks = interp_lon.reshape(N_LON, FLON, CLON + 2)
    rowwise = jnp.einsum('aip,lapbq->abliq', lat_blocks, windows, precision=HIGHEST)
    result = jnp.einsum('abliq,bjq->ablij', rowwise, lon_blocks, precision=HIGHEST)
    return result.reshape(N_LAT, N_LON, LEV * FLAT * FLON)

def reference(control, ens_pert, lat_filter, lon_filter, interp_lat, interp_lon, obs_cell, obs_count, obs_value, obs_weight):
    lat_matrix = lat_filter.astype(jnp.float32)
    lon_matrix = lon_filter.astype(jnp.float32)
    slot_range = jnp.arange(CAP).astype(jnp.int32)
    usable = (slot_range[None, None, None, None, :] < obs_count[..., None]).astype(jnp.float32)

    def arrange(table):
        return jnp.transpose(table, (1, 2, 3, 0, 4)).reshape(SLOTS, N_LAT, N_LON, N_TM * CAP)
    columns = arrange(obs_cell)
    targets = arrange(obs_value)
    weights = arrange(obs_weight * usable)

    def observe(source):
        spread = spread_both(source, lat_matrix, lon_matrix)

        def one_slot(inputs):
            members, places = inputs
            increment = lax.optimization_barrier(jnp.sum(spread * members.astype(jnp.float32), axis=0))
            finer = to_fine(increment, interp_lat, interp_lon)
            return jnp.take_along_axis(finer, places, axis=2)
        return lax.map(one_slot, (ens_pert, columns))
    values, pullback = jax.vjp(observe, control)
    departure = weights * (values - targets)
    adjoint, = pullback(departure)
    return control + adjoint
```

```python
import functools

import jax
import jax.numpy as jnp
from jax import lax
from jax.experimental import pallas as pl
from jax.experimental.pallas import tpu as pltpu
from jax.sharding import PartitionSpec as P

F32 = jnp.float32
BF16 = jnp.bfloat16
HIGHEST = lax.Precision.HIGHEST
MESH = pl.DeviceIdType.MESH
ROWS, COLS = 16, 128
FINE_ROWS, FINE_COLS = 32, 256
KR = 256


def halves(x):
    high = x.astype(BF16)
    return high, (x - high.astype(F32)).astype(BF16)


def nt(a, b, **kw):
    return lax.dot_general(a, b, (((1,), (1,)), ((), ())), preferred_element_type=F32, **kw)


def nn(a, b, **kw):
    return lax.dot_general(a, b, (((1,), (0,)), ((), ())), preferred_element_type=F32, **kw)


def kernel(
    NT,
    NL,
    ctl,
    pert,
    latf,
    lonf,
    ilat,
    ilon,
    opk,
    out,
    cs,
    pv,
    lf,
    nf,
    abuf,
    obuf,
    psend,
    pbuf,
    ybuf,
    bbuf,
    inc,
    rows,
    wown,
    woth,
    lr,
    wbuf,
    rtb,
    ctb,
    gb,
    grow,
    gown,
    goth,
    glr,
    hbuf,
    b2,
    adb,
    ap,
    lsem,
    ssem,
    rsem,
):
    t, i, j = lax.axis_index("tm"), lax.axis_index("lat"), lax.axis_index("lon")
    ch = j // 2
    rg = j % 2

    def send(src, dst, phase, where):
        pltpu.make_async_remote_copy(
            src_ref=src,
            dst_ref=dst,
            send_sem=ssem.at[phase],
            recv_sem=rsem.at[phase],
            device_id=where,
            device_id_type=MESH,
        ).start()

    def arrived(ref, phase):
        pltpu.make_async_copy(ref, ref, rsem.at[phase]).wait()

    def sent(ref, phase):
        pltpu.make_async_copy(ref, ref, ssem.at[phase]).wait()

    def loop(first, last, body):
        def step(k, carry):
            body(k)
            return carry

        lax.fori_loop(first, last, step, 0)

    c1 = pltpu.make_async_copy(ctl.at[:, t], cs, lsem.at[0])
    c2 = pltpu.make_async_copy(pert, pv, lsem.at[1])
    c3 = pltpu.make_async_copy(latf, lf, lsem.at[2])
    c4 = pltpu.make_async_copy(lonf.at[pl.ds(ch * 256, 256)], nf, lsem.at[3])
    c1.start()
    c2.start()
    c3.start()
    c4.start()
    c1.wait()

    def send_a(k):
        to = (i + k) % NL
        send(cs.at[to], abuf.at[i], 0, (t, to, j))

    loop(1, NL, send_a)
    abuf[i] = cs[i]

    def send_o(k):
        to = (t + k) % NT
        send(opk.at[to], obuf.at[t], 1, (to, i, j))

    loop(1, NT, send_o)
    obuf[t] = opk[t]

    c2.wait()

    def widen(l):
        x = pv[:, l].astype(F32)
        psend[l * 2] = x[:, :8]
        psend[l * 2 + 1] = x[:, 8:]

    loop(0, NT, widen)

    def send_p(k):
        to = (t + k // 2) % NT
        half = (rg + k) % 2
        send(psend.at[to * 2 + half], pbuf.at[t * 2 + rg], 2, (to, i, ch * 2 + half))

    loop(1, 2 * NT, send_p)
    pbuf[t * 2 + rg] = psend[t * 2 + rg]

    @pl.when(i == 0)
    def _():
        lr[: 4 * NT] = jnp.zeros((4 * NT, 1, COLS), F32)

    @pl.when(i == NL - 1)
    def _():
        lr[4 * NT :] = jnp.zeros((4 * NT, 1, COLS), F32)

    no_rim = jnp.logical_or(
        jnp.logical_and(rg == 0, i == 0), jnp.logical_and(rg == 1, i == NL - 1)
    )
    rim = jnp.logical_not(no_rim)

    @pl.when(no_rim)
    def _():
        glr[...] = jnp.zeros(glr.shape, F32)

    wbuf[...] = jnp.zeros(wbuf.shape, F32)

    k_row = lax.broadcasted_iota(jnp.int32, (KR, 18), 0)
    k_col = lax.broadcasted_iota(jnp.int32, (KR, 18), 1)
    inner = NT * 16
    place = jnp.where(
        k_row < inner,
        1 + (k_row & 15),
        jnp.where(k_row < inner + NT, 0, jnp.where(k_row < inner + 2 * NT, ROWS + 1, -1)),
    )
    pick = (place == k_col).astype(F32)
    p_rows = nt(pick, ilat[...], precision=HIGHEST)
    q_row = lax.broadcasted_iota(jnp.int32, (256, COLS + 2), 0)
    q_col = lax.broadcasted_iota(jnp.int32, (256, COLS + 2), 1)
    place = jnp.where(
        q_row < COLS, q_row + 1, jnp.where(q_row == 255, 0, jnp.where(q_row == COLS, COLS + 1, -1))
    )
    pick = (place == q_col).astype(F32)
    q_rows = nt(pick, ilon[...], precision=HIGHEST)
    arrived(obuf.at[pl.ds(0, NT - 1)], 1)
    lists = jnp.concatenate(
        [obuf[2 * k] + pltpu.roll(obuf[2 * k + 1], 64, 1) for k in range(NT // 2)], axis=1
    )
    n_obs = NT * 64
    cell = lists[0:1].astype(jnp.int32)
    target = lists[1:2]
    weight = lists[2:3]
    o_lev = cell >> 13
    o_row = (cell >> 8) & 31
    o_col = cell & 255
    hot_row = (lax.broadcasted_iota(jnp.int32, (FINE_ROWS, n_obs), 0) == o_row).astype(F32)
    hot_col = (lax.broadcasted_iota(jnp.int32, (FINE_COLS, n_obs), 0) == o_col).astype(F32)
    lev = lax.broadcasted_iota(jnp.int32, (KR, n_obs), 0)
    lev = jnp.where(lev < inner, lev >> 4, jnp.where(lev < inner + NT, lev - inner, lev - inner - NT))
    r_mat = nn(p_rows, hot_row, precision=HIGHEST)
    rtb[...] = jnp.where(lev == o_lev, r_mat, 0.0)
    ctb[...] = nn(q_rows, hot_col, precision=HIGHEST)

    c3.wait()
    c4.wait()
    lat_m = lf[...]
    lat_t = lat_m.astype(F32).T.astype(BF16)
    arrived(abuf.at[pl.ds(0, NL - 1)], 0)
    high, low = halves(abuf[...].reshape(NL * ROWS, COLS))
    both = nn(lat_m, jnp.concatenate([high, low], axis=1))
    ybuf[...] = (both[:, :COLS] + both[:, COLS:]).reshape(2 * NL, 8, COLS)

    def send_b(k):
        lat = (i + k // 4) % NL
        lon = (j + k) % 4
        send(ybuf.at[lat * 2 + lon % 2], bbuf.at[j * NL + i], 3, (t, lat, lon))

    loop(1, 4 * NL, send_b)
    bbuf[j * NL + i] = ybuf[i * 2 + rg]
    arrived(bbuf.at[pl.ds(0, 4 * NL - 1)], 3)

    m8 = NL * 8
    wide = jnp.concatenate(
        [bbuf[NL * b : NL * b + NL].reshape(m8, COLS) for b in range(4)], axis=1
    )
    lon_m = nf[...]
    both = nt(jnp.concatenate(halves(wide), axis=0), lon_m)
    z = both[:m8] + both[m8:]
    z0 = z[:, :COLS].reshape(NL, 8, COLS)
    z1 = z[:, COLS:].reshape(NL, 8, COLS)

    arrived(pbuf.at[pl.ds(0, 2 * NT - 1)], 2)

    for s in range(NT):
        for blk, zz in enumerate((z0, z1)):
            x = jnp.sum(zz * pbuf[2 * s + blk], axis=0)
            inc[2 * s + blk] = x
            rows[2 * s + blk] = jnp.where(rg == 0, x[0:1], x[7:8])

    def send_d(k):
        s = (t + k // 2) % NT
        lon = ch * 2 + (rg + k) % 2
        send(inc.at[pl.ds(2 * s, 2)], wown.at[pl.ds((t * 2 + rg) * 2, 2)], 4, (s, i, lon))

    loop(1, 2 * NT, send_d)

    def send_e(k):
        s = (t + k // 2) % NT
        e = k % 2
        send(inc.at[2 * s + 1 - e], woth.at[t * 2 + rg], 5, (s, i, 2 - 2 * ch + e))

    loop(0, 2 * NT, send_e)

    @pl.when(rim)
    def _():
        lat = i + 2 * rg - 1

        def send_f(k):
            s = (t + k // 4) % NT
            spot = ((1 - rg) * NT + t) * 4 + ch * 2
            send(rows.at[pl.ds(2 * s, 2)], lr.at[pl.ds(spot, 2)], 6 + rg, (s, lat, k % 4))

        loop(0, 4 * NT, send_f)

    wown[(t * 2 + rg) * 2] = inc[2 * t]
    wown[(t * 2 + rg) * 2 + 1] = inc[2 * t + 1]

    arrived(wown.at[pl.ds(0, 2 * (2 * NT - 1))], 4)
    arrived(woth, 5)

    @pl.when(i > 0)
    def _():
        arrived(lr.at[pl.ds(0, 4 * NT)], 7)

    @pl.when(i < NL - 1)
    def _():
        arrived(lr.at[pl.ds(4 * NT, 4 * NT)], 6)

    even = rg == 0
    w = wown[...].reshape(2 * NT, 2, 8, COLS)
    w0, w1 = w[:, 0].reshape(16 * NT, COLS), w[:, 1].reshape(16 * NT, COLS)
    lane = lax.broadcasted_iota(jnp.int32, (16 * NT, COLS), 1)
    near = jnp.where(even, 0, COLS - 1)
    far = COLS - 1 - near
    wbuf[:inner, :COLS] = jnp.where(even, w0, w1)
    wbuf[:inner, COLS:] = jnp.where(
        lane == near,
        jnp.where(even, w1, w0),
        jnp.where(lane == far, woth[...].reshape(16 * NT, COLS), 0.0),
    )
    lane1 = lax.broadcasted_iota(jnp.int32, (1, COLS), 1)
    for k in range(2 * NT):
        before = lr[k * 4 + (j + 3) % 4]
        after = lr[k * 4 + (j + 1) % 4]
        wbuf[inner + k : inner + k + 1, :COLS] = lr[k * 4 + j]
        wbuf[inner + k : inner + k + 1, COLS:] = jnp.where(
            lane1 == COLS - 1, before, jnp.where(lane1 == 0, after, 0.0)
        )

    r_high, r_low = halves(rtb[...])
    w_high, w_low = halves(wbuf[...].T)
    both = nn(jnp.concatenate([w_high, w_low], axis=0), r_high)
    mixed = both[:256] + both[256:] + nn(w_high, r_low)
    cols = ctb[...]
    seen = jnp.sum(mixed * cols, axis=0, keepdims=True)
    departure = weight * (seen - target)
    d_high, d_low = halves(cols * departure)
    both = nt(jnp.concatenate([r_high, r_low], axis=0), d_high)
    g = both[:KR] + both[KR:] + nt(r_high, d_low)
    for k in range(2 * NT):
        gb[2 * k] = g[8 * k : 8 * k + 8, :COLS]
        gb[2 * k + 1] = g[8 * k : 8 * k + 8, COLS:]
    for k in range(2 * NT):
        grow[2 * k] = g[inner + k : inner + k + 1, :COLS]
        grow[2 * k + 1] = g[inner + k : inner + k + 1, COLS:]

    def send_g(k):
        l = (t + k // 2) % NT
        half = (rg + k) % 2
        send(
            gb.at[pl.ds((l * 2 + half) * 2, 2)],
            gown.at[pl.ds((t * 2 + rg) * 2, 2)],
            8,
            (l, i, ch * 2 + half),
        )

    loop(1, 2 * NT, send_g)

    def send_h(k):
        l = (t + k // 2) % NT
        half = k % 2
        send(
            gb.at[(l * 2 + half) * 2 + 1], goth.at[t * 2 + rg], 9, (l, i, 2 - 2 * ch + half)
        )

    loop(0, 2 * NT, send_h)

    def send_rim(pos):
        def go(k):
            l = (t + k // 2) % NT
            send(
                grow.at[pl.ds((pos * NT + l) * 2, 2)],
                glr.at[pl.ds((t * 4 + j) * 2, 2)],
                10 + pos,
                (l, i - 1 + 2 * pos, (k % 2) * 2 + 1 - pos),
            )

        loop(0, 2 * NT, go)

    @pl.when(i > 0)
    def _():
        send_rim(0)

    @pl.when(i < NL - 1)
    def _():
        send_rim(1)

    gown[(t * 2 + rg) * 2] = gb[(t * 2 + rg) * 2]
    gown[(t * 2 + rg) * 2 + 1] = gb[(t * 2 + rg) * 2 + 1]
    arrived(gown.at[pl.ds(0, 2 * (2 * NT - 1))], 8)
    arrived(goth, 9)

    @pl.when(jnp.logical_and(rim, rg == 1))
    def _():
        arrived(glr, 10)

    @pl.when(jnp.logical_and(rim, rg == 0))
    def _():
        arrived(glr, 11)

    lane8 = lax.broadcasted_iota(jnp.int32, (8, COLS), 1)
    row8 = lax.broadcasted_iota(jnp.int32, (8, COLS), 0)
    first, last = lane8 == 0, lane8 == COLS - 1
    mine = row8 == jnp.where(even, 0, 7)
    other = 2 - 2 * ch
    acc0 = acc1 = None
    for s in range(NT):
        def rim_of(b, part, s=s):
            return jnp.broadcast_to(glr[(s * 4 + b) * 2 + part], (8, COLS))

        d0 = gown[s * 4] + jnp.where(last, gown[s * 4 + 3], 0.0)
        d0 = d0 + jnp.where(first, goth[s * 2 + 1], 0.0)
        e0 = rim_of(ch * 2, 0) + jnp.where(last, rim_of(ch * 2 + 1, 1), 0.0)
        e0 = e0 + jnp.where(first, rim_of(other + 1, 1), 0.0)
        d0 = d0 + jnp.where(mine, e0, 0.0)
        d1 = gown[s * 4 + 2] + jnp.where(first, gown[s * 4 + 1], 0.0)
        d1 = d1 + jnp.where(last, goth[s * 2], 0.0)
        e1 = rim_of(ch * 2 + 1, 0) + jnp.where(first, rim_of(ch * 2, 1), 0.0)
        e1 = e1 + jnp.where(last, rim_of(other, 1), 0.0)
        d1 = d1 + jnp.where(mine, e1, 0.0)
        p0, p1 = pbuf[2 * s] * d0[None], pbuf[2 * s + 1] * d1[None]
        acc0, acc1 = (p0, p1) if s == 0 else (acc0 + p0, acc1 + p1)
    grad = jnp.concatenate([acc0.reshape(m8, COLS), acc1.reshape(m8, COLS)], axis=1)
    both = nn(jnp.concatenate(halves(grad), axis=0), lon_m)
    h = both[:m8] + both[m8:]
    for b in range(4):
        hbuf[NL * b : NL * b + NL] = h[:, b * COLS : (b + 1) * COLS].reshape(NL, 8, COLS)

    def send_c(k):
        lat = (i + k // 4) % NL
        lon = (j + k) % 4
        send(hbuf.at[lon * NL + lat], b2.at[ch * 2 * NL + 2 * i + rg], 12, (t, lat, lon))

    loop(1, 4 * NL, send_c)
    b2[ch * 2 * NL + 2 * i + rg] = hbuf[j * NL + i]
    arrived(b2.at[pl.ds(0, 4 * NL - 1)], 12)
    y = (b2[: 2 * NL] + b2[2 * NL :]).reshape(NL * ROWS, COLS)
    high, low = halves(y)
    both = nn(lat_t, jnp.concatenate([high, low], axis=1))
    adb[...] = (both[:, :COLS] + both[:, COLS:]).reshape(NL, ROWS, COLS)

    def send_i(k):
        to = (i + k) % NL
        send(adb.at[to], ap.at[i], 13, (t, to, j))

    loop(1, NL, send_i)
    ap[i] = adb[i]
    arrived(ap.at[pl.ds(0, NL - 1)], 13)

    def send_j(k):
        send(ap, out.at[:, t], 14, ((t + k) % NT, i, j))

    loop(1, NT, send_j)
    last_copy = pltpu.make_async_copy(ap, out.at[:, t], lsem.at[0])
    last_copy.start()
    last_copy.wait()
    arrived(out.at[:, pl.ds(0, NT - 1)], 14)

    sent(abuf.at[pl.ds(0, NL - 1)], 0)
    sent(obuf.at[pl.ds(0, NT - 1)], 1)
    sent(pbuf.at[pl.ds(0, 2 * NT - 1)], 2)
    sent(bbuf.at[pl.ds(0, 4 * NL - 1)], 3)
    sent(wown.at[pl.ds(0, 2 * (2 * NT - 1))], 4)
    sent(woth, 5)

    @pl.when(jnp.logical_and(rim, rg == 0))
    def _():
        sent(glr, 6)

    @pl.when(jnp.logical_and(rim, rg == 1))
    def _():
        sent(glr, 7)

    sent(gown.at[pl.ds(0, 2 * (2 * NT - 1))], 8)
    sent(goth, 9)

    @pl.when(i > 0)
    def _():
        sent(lr.at[pl.ds(0, 4 * NT)], 10)

    @pl.when(i < NL - 1)
    def _():
        sent(lr.at[pl.ds(0, 4 * NT)], 11)

    sent(b2.at[pl.ds(0, 4 * NL - 1)], 12)
    sent(ap.at[pl.ds(0, NL - 1)], 13)
    sent(out.at[:, pl.ds(0, NT - 1)], 14)


def per_device(NT, NL, control, pert, latf, lonf, ilat, ilon, cell, count, value, weight):
    cap = cell.shape[-1]
    usable = (jnp.arange(cap) < count[0, :, 0, 0, None]).astype(F32)
    lists = jnp.stack(
        [cell[0, :, 0, 0].astype(F32), value[0, :, 0, 0], weight[0, :, 0, 0] * usable], axis=1
    )
    lists = jnp.pad(lists, ((0, 0), (0, 5), (0, COLS - cap)))
    any_space = pl.BlockSpec(memory_space=pl.ANY)
    vmem = pl.BlockSpec(memory_space=pltpu.VMEM)
    V = pltpu.VMEM
    tile = (8, COLS)
    scratch = [
        V((NL, ROWS, COLS), F32),
        V((NL, NT, ROWS, COLS), BF16),
        V((NL * ROWS, NL * ROWS), BF16),
        V((256, 512), BF16),
        V((NL, ROWS, COLS), F32),
        V((NT, *tile), F32),
        V((2 * NT, NL, *tile), F32),
        V((2 * NT, NL, *tile), F32),
        V((2 * NL, *tile), F32),
        V((4 * NL, *tile), F32),
        V((2 * NT, *tile), F32),
        V((2 * NT, 1, COLS), F32),
        V((4 * NT, *tile), F32),
        V((2 * NT, *tile), F32),
        V((8 * NT, 1, COLS), F32),
        V((KR, 256), F32),
        V((KR, NT * 64), F32),
        V((256, NT * 64), F32),
        V((4 * NT, *tile), F32),
        V((4 * NT, 1, COLS), F32),
        V((4 * NT, *tile), F32),
        V((2 * NT, *tile), F32),
        V((8 * NT, 1, COLS), F32),
        V((4 * NL, *tile), F32),
        V((4 * NL, *tile), F32),
        V((NL, ROWS, COLS), F32),
        V((NL, ROWS, COLS), F32),
        pltpu.SemaphoreType.DMA((4,)),
        pltpu.SemaphoreType.DMA((15,)),
        pltpu.SemaphoreType.DMA((15,)),
    ]
    adjoint = pl.pallas_call(
        functools.partial(kernel, NT, NL),
        name="gradient",
        out_shape=jax.ShapeDtypeStruct(control.shape, F32),
        in_specs=[any_space] * 4 + [vmem] * 3,
        out_specs=any_space,
        scratch_shapes=scratch,
        compiler_params=pltpu.CompilerParams(
            has_side_effects=True, vmem_limit_bytes=24 * 1024 * 1024
        ),
    )(control, pert[0], latf, lonf, ilat, ilon, lists)
    return control + adjoint


def solution(mesh):
    placed = (
        P(None, None, "lat", "lon"),
        P("tm", None, None, "lat", "lon"),
        P(),
        P(),
        P("lat", None),
        P("lon", None),
        P("tm", None, "lat", "lon", None),
        P("tm", None, "lat", "lon"),
        P("tm", None, "lat", "lon", None),
        P("tm", None, "lat", "lon", None),
    )
    return jax.shard_map(
        functools.partial(per_device, mesh.shape["tm"], mesh.shape["lat"]),
        mesh=mesh,
        in_specs=placed,
        out_specs=P(None, None, "lat", "lon"),
        check_vma=False,
    )
```

```python
import functools

import jax
import jax.numpy as jnp
from jax import lax
from jax.experimental import pallas as pl
from jax.experimental.pallas import tpu as pltpu
from jax.sharding import PartitionSpec as P

F32 = jnp.float32
BF16 = jnp.bfloat16
HIGHEST = lax.Precision.HIGHEST
MESH = pl.DeviceIdType.MESH
ROWS, COLS = 16, 128
FINE_ROWS, FINE_COLS = 32, 256
KR = 256


def halves(x):
    high = x.astype(BF16)
    return high, (x - high.astype(F32)).astype(BF16)


def nt(a, b, **kw):
    return lax.dot_general(a, b, (((1,), (1,)), ((), ())), preferred_element_type=F32, **kw)


def nn(a, b, **kw):
    return lax.dot_general(a, b, (((1,), (0,)), ((), ())), preferred_element_type=F32, **kw)


def kernel(
    NT,
    NL,
    ctl,
    pert,
    latf,
    lonf,
    ilat,
    ilon,
    o_cell,
    o_count,
    o_value,
    o_weight,
    out,
    vlat,
    vlon,
    vcell,
    vcount,
    vvalue,
    vweight,
    opk,
    cs,
    pv,
    lf,
    nf,
    abuf,
    obuf,
    psend,
    pbuf,
    ybuf,
    bbuf,
    inc,
    rows,
    wown,
    woth,
    lr,
    wbuf,
    rtb,
    ctb,
    gb,
    grow,
    gown,
    goth,
    glr,
    hbuf,
    b2,
    adb,
    lsem,
    ssem,
    rsem,
    hsem,
):
    t, i, j = lax.axis_index("tm"), lax.axis_index("lat"), lax.axis_index("lon")
    ch = j // 2
    rg = j % 2

    def send(src, dst, phase, where):
        pltpu.make_async_remote_copy(
            src_ref=src,
            dst_ref=dst,
            send_sem=ssem.at[phase],
            recv_sem=rsem.at[phase],
            device_id=where,
            device_id_type=MESH,
        ).start()

    def arrived(ref, phase):
        pltpu.make_async_copy(ref, ref, rsem.at[phase]).wait()

    def sent(ref, phase):
        pltpu.make_async_copy(ref, ref, ssem.at[phase]).wait()

    def loop(first, last, body):
        def step(k, carry):
            body(k)
            return carry

        lax.fori_loop(first, last, step, 0)

    copies = [
        pltpu.make_async_copy(src, dst, lsem.at[n])
        for n, (src, dst) in enumerate(
            (
                (pert, pv),
                (ilat, vlat),
                (ilon, vlon),
                (o_cell, vcell),
                (o_count, vcount),
                (o_value, vvalue),
                (o_weight, vweight),
                (ctl.at[:, t], cs),
                (latf, lf),
                (lonf.at[pl.ds(ch * 256, 256)], nf),
            )
        )
    ]
    for copy in copies:
        copy.start()

    ready = pltpu.get_barrier_semaphore()

    def hello(*where):
        pl.semaphore_signal(ready, inc=1, device_id=where, device_id_type=MESH)

    loop(1, 4 * NL, lambda k: hello(t, (i + k // 4) % NL, (j + k) % 4))
    loop(4, 4 * NT, lambda k: hello((t + k // 4) % NT, i, (j + k) % 4))

    @pl.when(i < NL - 1)
    def _():
        loop(2, 2 * NT, lambda k: hello((t + k // 2) % NT, i + 1, (k % 2) * 2))

        @pl.when(rg == 1)
        def _():
            loop(2, 2 * NT, lambda k: hello((t + k // 2) % NT, i + 1, (k % 2) * 2 + 1))

    @pl.when(i > 0)
    def _():
        loop(2, 2 * NT, lambda k: hello((t + k // 2) % NT, i - 1, (k % 2) * 2 + 1))

        @pl.when(rg == 0)
        def _():
            loop(2, 2 * NT, lambda k: hello((t + k // 2) % NT, i - 1, (k % 2) * 2))

    peers = 4 * NL - 1 + 4 * NT - 4
    peers = peers + jnp.where(i < NL - 1, (NT - 1) * (2 + 2 * rg), 0)
    peers = peers + jnp.where(i > 0, (NT - 1) * (4 - 2 * rg), 0)

    copies[0].wait()

    def widen(l):
        x = pv[:, l].astype(F32)
        psend[l * 2] = x[:, :8]
        psend[l * 2 + 1] = x[:, 8:]

    loop(0, NT, widen)
    for copy in copies[1:7]:
        copy.wait()
    opk[...] = jnp.zeros(opk.shape, F32)
    slot_entry = lax.broadcasted_iota(jnp.int32, (1, 64), 1)
    for s in range(NT):
        usable = slot_entry < vcount[0:1, s : s + 1]
        opk[s, 0:1, :64] = vcell[s].astype(F32)
        opk[s, 1:2, :64] = vvalue[s]
        opk[s, 2:3, :64] = jnp.where(usable, vweight[s], 0.0)

    @pl.when(i == 0)
    def _():
        lr[: 4 * NT] = jnp.zeros((4 * NT, 1, COLS), F32)

    @pl.when(i == NL - 1)
    def _():
        lr[4 * NT :] = jnp.zeros((4 * NT, 1, COLS), F32)

    no_rim = jnp.logical_or(
        jnp.logical_and(rg == 0, i == 0), jnp.logical_and(rg == 1, i == NL - 1)
    )
    rim = jnp.logical_not(no_rim)

    @pl.when(no_rim)
    def _():
        glr[...] = jnp.zeros(glr.shape, F32)

    wbuf[...] = jnp.zeros(wbuf.shape, F32)
    for copy in copies[7:]:
        copy.wait()
    lat_m = lf[...]
    lat_t = lat_m.astype(F32).T.astype(BF16)
    pl.semaphore_wait(ready, peers)

    def send_a(k):
        to = (i + k) % NL
        send(cs.at[to], abuf.at[i], 0, (t, to, j))

    loop(1, NL, send_a)
    abuf[i] = cs[i]

    def send_o(k):
        to = (t + k) % NT
        send(opk.at[to], obuf.at[t], 1, (to, i, j))

    loop(1, NT, send_o)
    obuf[t] = opk[t]

    def send_p(k):
        to = (t + k // 2) % NT
        half = (rg + k) % 2
        send(psend.at[to * 2 + half], pbuf.at[t * 2 + rg], 2, (to, i, ch * 2 + half))

    loop(1, 2 * NT, send_p)
    pbuf[t * 2 + rg] = psend[t * 2 + rg]

    k_row = lax.broadcasted_iota(jnp.int32, (KR, 18), 0)
    k_col = lax.broadcasted_iota(jnp.int32, (KR, 18), 1)
    inner = NT * 16
    place = jnp.where(
        k_row < inner,
        1 + (k_row & 15),
        jnp.where(k_row < inner + NT, 0, jnp.where(k_row < inner + 2 * NT, ROWS + 1, -1)),
    )
    pick = (place == k_col).astype(F32)
    p_rows = nn(pick, vlat[...], precision=HIGHEST)
    q_row = lax.broadcasted_iota(jnp.int32, (256, COLS + 2), 0)
    q_col = lax.broadcasted_iota(jnp.int32, (256, COLS + 2), 1)
    place = jnp.where(
        q_row < COLS, q_row + 1, jnp.where(q_row == 255, 0, jnp.where(q_row == COLS, COLS + 1, -1))
    )
    pick = (place == q_col).astype(F32)
    q_rows = nn(pick, vlon[...], precision=HIGHEST)
    arrived(obuf.at[pl.ds(0, NT - 1)], 1)
    lists = jnp.concatenate(
        [obuf[2 * k] + pltpu.roll(obuf[2 * k + 1], 64, 1) for k in range(NT // 2)], axis=1
    )
    n_obs = NT * 64
    cell = lists[0:1].astype(jnp.int32)
    target = lists[1:2]
    weight = lists[2:3]
    o_lev = cell >> 13
    o_row = (cell >> 8) & 31
    o_col = cell & 255
    hot_row = (lax.broadcasted_iota(jnp.int32, (FINE_ROWS, n_obs), 0) == o_row).astype(F32)
    hot_col = (lax.broadcasted_iota(jnp.int32, (FINE_COLS, n_obs), 0) == o_col).astype(F32)
    lev = lax.broadcasted_iota(jnp.int32, (KR, n_obs), 0)
    lev = jnp.where(lev < inner, lev >> 4, jnp.where(lev < inner + NT, lev - inner, lev - inner - NT))
    r_mat = nn(p_rows, hot_row, precision=HIGHEST)
    rtb[...] = jnp.where(lev == o_lev, r_mat, 0.0)
    ctb[...] = nn(q_rows, hot_col, precision=HIGHEST)

    arrived(abuf.at[pl.ds(0, NL - 1)], 0)
    high, low = halves(abuf[...].reshape(NL * ROWS, COLS))
    both = nn(lat_m, jnp.concatenate([high, low], axis=1))
    ybuf[...] = (both[:, :COLS] + both[:, COLS:]).reshape(2 * NL, 8, COLS)

    def send_b(k):
        lat = (i + k // 4) % NL
        lon = (j + k) % 4
        send(ybuf.at[lat * 2 + lon % 2], bbuf.at[j * NL + i], 3, (t, lat, lon))

    loop(1, 4 * NL, send_b)
    bbuf[j * NL + i] = ybuf[i * 2 + rg]
    arrived(bbuf.at[pl.ds(0, 4 * NL - 1)], 3)

    m8 = NL * 8
    wide = jnp.concatenate(
        [bbuf[NL * b : NL * b + NL].reshape(m8, COLS) for b in range(4)], axis=1
    )
    lon_m = nf[...]
    both = nt(jnp.concatenate(halves(wide), axis=0), lon_m)
    z = both[:m8] + both[m8:]
    z0 = z[:, :COLS].reshape(NL, 8, COLS)
    z1 = z[:, COLS:].reshape(NL, 8, COLS)

    arrived(pbuf.at[pl.ds(0, 2 * NT - 1)], 2)

    for s in range(NT):
        for blk, zz in enumerate((z0, z1)):
            x = jnp.sum(zz * pbuf[2 * s + blk], axis=0)
            inc[2 * s + blk] = x
            rows[2 * s + blk] = jnp.where(rg == 0, x[0:1], x[7:8])

    def send_d(k):
        s = (t + k // 2) % NT
        lon = ch * 2 + (rg + k) % 2
        send(inc.at[pl.ds(2 * s, 2)], wown.at[pl.ds((t * 2 + rg) * 2, 2)], 4, (s, i, lon))

    loop(1, 2 * NT, send_d)

    def send_e(k):
        s = (t + k // 2) % NT
        e = k % 2
        send(inc.at[2 * s + 1 - e], woth.at[t * 2 + rg], 5, (s, i, 2 - 2 * ch + e))

    loop(0, 2 * NT, send_e)

    @pl.when(rim)
    def _():
        lat = i + 2 * rg - 1

        def send_f(k):
            s = (t + k // 4) % NT
            spot = ((1 - rg) * NT + t) * 4 + ch * 2
            send(rows.at[pl.ds(2 * s, 2)], lr.at[pl.ds(spot, 2)], 6 + rg, (s, lat, k % 4))

        loop(0, 4 * NT, send_f)

    wown[(t * 2 + rg) * 2] = inc[2 * t]
    wown[(t * 2 + rg) * 2 + 1] = inc[2 * t + 1]

    arrived(wown.at[pl.ds(0, 2 * (2 * NT - 1))], 4)
    arrived(woth, 5)

    @pl.when(i > 0)
    def _():
        arrived(lr.at[pl.ds(0, 4 * NT)], 7)

    @pl.when(i < NL - 1)
    def _():
        arrived(lr.at[pl.ds(4 * NT, 4 * NT)], 6)

    even = rg == 0
    w = wown[...].reshape(2 * NT, 2, 8, COLS)
    w0, w1 = w[:, 0].reshape(16 * NT, COLS), w[:, 1].reshape(16 * NT, COLS)
    lane = lax.broadcasted_iota(jnp.int32, (16 * NT, COLS), 1)
    near = jnp.where(even, 0, COLS - 1)
    far = COLS - 1 - near
    wbuf[:inner, :COLS] = jnp.where(even, w0, w1)
    wbuf[:inner, COLS:] = jnp.where(
        lane == near,
        jnp.where(even, w1, w0),
        jnp.where(lane == far, woth[...].reshape(16 * NT, COLS), 0.0),
    )
    lane1 = lax.broadcasted_iota(jnp.int32, (1, COLS), 1)
    for k in range(2 * NT):
        before = lr[k * 4 + (j + 3) % 4]
        after = lr[k * 4 + (j + 1) % 4]
        wbuf[inner + k : inner + k + 1, :COLS] = lr[k * 4 + j]
        wbuf[inner + k : inner + k + 1, COLS:] = jnp.where(
            lane1 == COLS - 1, before, jnp.where(lane1 == 0, after, 0.0)
        )

    r_high, r_low = halves(rtb[...])
    w_high, w_low = halves(wbuf[...].T)
    both = nn(jnp.concatenate([w_high, w_low], axis=0), r_high)
    mixed = both[:256] + both[256:] + nn(w_high, r_low)
    cols = ctb[...]
    seen = jnp.sum(mixed * cols, axis=0, keepdims=True)
    departure = weight * (seen - target)
    d_high, d_low = halves(cols * departure)
    both = nt(jnp.concatenate([r_high, r_low], axis=0), d_high)
    g = both[:KR] + both[KR:] + nt(r_high, d_low)
    for k in range(2 * NT):
        gb[2 * k] = g[8 * k : 8 * k + 8, :COLS]
        gb[2 * k + 1] = g[8 * k : 8 * k + 8, COLS:]
    for k in range(2 * NT):
        grow[2 * k] = g[inner + k : inner + k + 1, :COLS]
        grow[2 * k + 1] = g[inner + k : inner + k + 1, COLS:]

    def send_g(k):
        l = (t + k // 2) % NT
        half = (rg + k) % 2
        send(
            gb.at[pl.ds((l * 2 + half) * 2, 2)],
            gown.at[pl.ds((t * 2 + rg) * 2, 2)],
            8,
            (l, i, ch * 2 + half),
        )

    loop(1, 2 * NT, send_g)

    def send_h(k):
        l = (t + k // 2) % NT
        half = k % 2
        send(
            gb.at[(l * 2 + half) * 2 + 1], goth.at[t * 2 + rg], 9, (l, i, 2 - 2 * ch + half)
        )

    loop(0, 2 * NT, send_h)

    def send_rim(pos):
        def go(k):
            l = (t + k // 2) % NT
            send(
                grow.at[pl.ds((pos * NT + l) * 2, 2)],
                glr.at[pl.ds((t * 4 + j) * 2, 2)],
                10 + pos,
                (l, i - 1 + 2 * pos, (k % 2) * 2 + 1 - pos),
            )

        loop(0, 2 * NT, go)

    @pl.when(i > 0)
    def _():
        send_rim(0)

    @pl.when(i < NL - 1)
    def _():
        send_rim(1)

    gown[(t * 2 + rg) * 2] = gb[(t * 2 + rg) * 2]
    gown[(t * 2 + rg) * 2 + 1] = gb[(t * 2 + rg) * 2 + 1]
    arrived(gown.at[pl.ds(0, 2 * (2 * NT - 1))], 8)
    arrived(goth, 9)

    @pl.when(jnp.logical_and(rim, rg == 1))
    def _():
        arrived(glr, 10)

    @pl.when(jnp.logical_and(rim, rg == 0))
    def _():
        arrived(glr, 11)

    lane8 = lax.broadcasted_iota(jnp.int32, (8, COLS), 1)
    row8 = lax.broadcasted_iota(jnp.int32, (8, COLS), 0)
    first, last = lane8 == 0, lane8 == COLS - 1
    mine = row8 == jnp.where(even, 0, 7)
    other = 2 - 2 * ch
    acc0 = acc1 = None
    for s in range(NT):
        def rim_of(b, part, s=s):
            return jnp.broadcast_to(glr[(s * 4 + b) * 2 + part], (8, COLS))

        d0 = gown[s * 4] + jnp.where(last, gown[s * 4 + 3], 0.0)
        d0 = d0 + jnp.where(first, goth[s * 2 + 1], 0.0)
        e0 = rim_of(ch * 2, 0) + jnp.where(last, rim_of(ch * 2 + 1, 1), 0.0)
        e0 = e0 + jnp.where(first, rim_of(other + 1, 1), 0.0)
        d0 = d0 + jnp.where(mine, e0, 0.0)
        d1 = gown[s * 4 + 2] + jnp.where(first, gown[s * 4 + 1], 0.0)
        d1 = d1 + jnp.where(last, goth[s * 2], 0.0)
        e1 = rim_of(ch * 2 + 1, 0) + jnp.where(first, rim_of(ch * 2, 1), 0.0)
        e1 = e1 + jnp.where(last, rim_of(other, 1), 0.0)
        d1 = d1 + jnp.where(mine, e1, 0.0)
        p0, p1 = pbuf[2 * s] * d0[None], pbuf[2 * s + 1] * d1[None]
        acc0, acc1 = (p0, p1) if s == 0 else (acc0 + p0, acc1 + p1)
    grad = jnp.concatenate([acc0.reshape(m8, COLS), acc1.reshape(m8, COLS)], axis=1)
    both = nn(jnp.concatenate(halves(grad), axis=0), lon_m)
    h = both[:m8] + both[m8:]
    for b in range(4):
        hbuf[NL * b : NL * b + NL] = h[:, b * COLS : (b + 1) * COLS].reshape(NL, 8, COLS)

    def send_c(k):
        lat = (i + k // 4) % NL
        lon = (j + k) % 4
        send(hbuf.at[lon * NL + lat], b2.at[ch * 2 * NL + 2 * i + rg], 12, (t, lat, lon))

    loop(1, 4 * NL, send_c)
    b2[ch * 2 * NL + 2 * i + rg] = hbuf[j * NL + i]
    arrived(b2.at[pl.ds(0, 4 * NL - 1)], 12)
    y = (b2[: 2 * NL] + b2[2 * NL :]).reshape(NL * ROWS, COLS)
    high, low = halves(y)
    both = nn(lat_t, jnp.concatenate([high, low], axis=1))
    adb[...] = (both[:, :COLS] + both[:, COLS:]).reshape(NL, ROWS, COLS)

    chunks = 4 if NL % 4 == 0 else NL
    size = NL // chunks
    own = i // size

    def send_i(k):
        to = (i + k) % NL
        send(adb.at[to], out.at[i, t], 16 + own, (t, to, j))

    loop(1, NL, send_i)
    out[i, t] = adb[i]

    core = t % 2
    sibling = t + 1 - 2 * core
    right, left = (t + 2) % NT, (t + NT - 2) % NT
    chips = NT // 2
    order = (0, 1, 3, 2) if chunks == 4 else tuple(range(chunks))
    places = [(own + o) % chunks for o in order]

    def chunk(q, owner):
        return out.at[pl.ds(q * size, size), owner]

    def pass_on(q, owner, n, to):
        pltpu.make_async_remote_copy(
            src_ref=chunk(q, owner),
            dst_ref=chunk(q, owner),
            send_sem=ssem.at[14],
            recv_sem=hsem.at[n],
            device_id=(to, i, j),
            device_id_type=MESH,
        ).start()

    def landed(q, n):
        pltpu.make_async_copy(chunk(q, t), chunk(q, t), hsem.at[n]).wait()

    from_left, from_right, from_far, from_sibling = 0, chunks, 2 * chunks, 3 * chunks

    def relay(k):
        q = places[k]
        landed(q, from_left + k)
        if 2 * k < chunks:
            pass_on(q, left, from_far + k, right)
        pass_on(q, left, from_sibling, sibling)
        landed(q, from_right + k)
        if 2 * k >= chunks:
            pass_on(q, right, from_far + k, left)
        pass_on(q, right, from_sibling, sibling)

    for k, q in enumerate(places):
        if k == 0:
            if size > 1:
                arrived(out.at[pl.ds(0, size - 1), t], 16 + q)
        else:
            arrived(out.at[pl.ds(0, size), t], 16 + q)
        if chips > 1:
            pass_on(q, t, from_left + k, right)
            pass_on(q, t, from_right + k, left)
        pass_on(q, t, from_sibling, sibling)
        if chips > 1 and k > 0:
            relay(k - 1)
    if chips > 1:
        relay(chunks - 1)
        across = (t + NT // 2) % NT
        for k, q in enumerate(places):
            landed(q, from_far + k)
            pass_on(q, across, from_sibling, sibling)
    everything = out.at[:, pl.ds(0, chips)]
    pltpu.make_async_copy(everything, everything, hsem.at[from_sibling]).wait()

    sent(abuf.at[pl.ds(0, NL - 1)], 0)
    sent(obuf.at[pl.ds(0, NT - 1)], 1)
    sent(pbuf.at[pl.ds(0, 2 * NT - 1)], 2)
    sent(bbuf.at[pl.ds(0, 4 * NL - 1)], 3)
    sent(wown.at[pl.ds(0, 2 * (2 * NT - 1))], 4)
    sent(woth, 5)

    @pl.when(jnp.logical_and(rim, rg == 0))
    def _():
        sent(glr, 6)

    @pl.when(jnp.logical_and(rim, rg == 1))
    def _():
        sent(glr, 7)

    sent(gown.at[pl.ds(0, 2 * (2 * NT - 1))], 8)
    sent(goth, 9)

    @pl.when(i > 0)
    def _():
        sent(lr.at[pl.ds(0, 4 * NT)], 10)

    @pl.when(i < NL - 1)
    def _():
        sent(lr.at[pl.ds(0, 4 * NT)], 11)

    sent(b2.at[pl.ds(0, 4 * NL - 1)], 12)
    sent(out.at[pl.ds(0, NL - 1), t], 16 + own)
    sent(out.at[:, pl.ds(0, NT - 1)], 14)


def per_device(NT, NL, control, pert, latf, lonf, ilat, ilon, cell, count, value, weight):
    hbm = pl.BlockSpec(memory_space=pltpu.HBM)
    V = pltpu.VMEM
    tile = (8, COLS)
    cap = cell.shape[-1]
    scratch = [
        V((ROWS + 2, FINE_ROWS), F32),
        V((COLS + 2, FINE_COLS), F32),
        V((NT, 1, cap), jnp.int32),
        V((1, NT), jnp.int32),
        V((NT, 1, cap), F32),
        V((NT, 1, cap), F32),
        V((NT, *tile), F32),
        V((NL, ROWS, COLS), F32),
        V((NL, NT, ROWS, COLS), BF16),
        V((NL * ROWS, NL * ROWS), BF16),
        V((256, 512), BF16),
        V((NL, ROWS, COLS), F32),
        V((NT, *tile), F32),
        V((2 * NT, NL, *tile), F32),
        V((2 * NT, NL, *tile), F32),
        V((2 * NL, *tile), F32),
        V((4 * NL, *tile), F32),
        V((2 * NT, *tile), F32),
        V((2 * NT, 1, COLS), F32),
        V((4 * NT, *tile), F32),
        V((2 * NT, *tile), F32),
        V((8 * NT, 1, COLS), F32),
        V((KR, 256), F32),
        V((KR, NT * 64), F32),
        V((256, NT * 64), F32),
        V((4 * NT, *tile), F32),
        V((4 * NT, 1, COLS), F32),
        V((4 * NT, *tile), F32),
        V((2 * NT, *tile), F32),
        V((8 * NT, 1, COLS), F32),
        V((4 * NL, *tile), F32),
        V((4 * NL, *tile), F32),
        V((NL, ROWS, COLS), F32),
        pltpu.SemaphoreType.DMA((10,)),
        pltpu.SemaphoreType.DMA((20,)),
        pltpu.SemaphoreType.DMA((20,)),
        pltpu.SemaphoreType.DMA((13,)),
    ]
    adjoint = pl.pallas_call(
        functools.partial(kernel, NT, NL),
        name="gradient",
        out_shape=jax.ShapeDtypeStruct(control.shape, F32),
        in_specs=[hbm] * 10,
        out_specs=pl.BlockSpec(memory_space=pltpu.VMEM),
        scratch_shapes=scratch,
        compiler_params=pltpu.CompilerParams(
            has_side_effects=True, collective_id=0, vmem_limit_bytes=63 * 1024 * 1024
        ),
    )(
        control,
        pert[0],
        latf,
        lonf,
        ilat.T,
        ilon.T,
        cell.reshape(NT, 1, cap),
        count.reshape(1, NT),
        value.reshape(NT, 1, cap),
        weight.reshape(NT, 1, cap),
    )
    return control + adjoint


def solution(mesh):
    placed = (
        P(None, None, "lat", "lon"),
        P("tm", None, None, "lat", "lon"),
        P(),
        P(),
        P("lat", None),
        P("lon", None),
        P("tm", None, "lat", "lon", None),
        P("tm", None, "lat", "lon"),
        P("tm", None, "lat", "lon", None),
        P("tm", None, "lat", "lon", None),
    )
    return jax.shard_map(
        functools.partial(per_device, mesh.shape["tm"], mesh.shape["lat"]),
        mesh=mesh,
        in_specs=placed,
        out_specs=P(None, None, "lat", "lon"),
        check_vma=False,
    )
```

```python
import functools

import jax
import jax.numpy as jnp
from jax import lax
from jax.experimental import pallas as pl
from jax.experimental.pallas import tpu as pltpu
from jax.sharding import PartitionSpec as P

F32 = jnp.float32
BF16 = jnp.bfloat16
HIGHEST = lax.Precision.HIGHEST
MESH = pl.DeviceIdType.MESH
ROWS, COLS = 16, 128
FINE_ROWS, FINE_COLS = 32, 256
KR = 256


def halves(x):
    high = x.astype(BF16)
    return high, (x - high.astype(F32)).astype(BF16)


def nt(a, b, **kw):
    return lax.dot_general(a, b, (((1,), (1,)), ((), ())), preferred_element_type=F32, **kw)


def nn(a, b, **kw):
    return lax.dot_general(a, b, (((1,), (0,)), ((), ())), preferred_element_type=F32, **kw)


def kernel(
    NT,
    NL,
    ctl,
    pert,
    latf,
    lonf,
    ilat,
    ilon,
    o_cell,
    o_count,
    o_value,
    o_weight,
    out,
    vlat,
    vlon,
    vcell,
    vcount,
    vvalue,
    vweight,
    opk,
    cs,
    pv,
    lf,
    nf,
    abuf,
    obuf,
    psend,
    pbuf,
    ybuf,
    bbuf,
    inc,
    rows,
    wown,
    woth,
    lr,
    wbuf,
    rtb,
    ctb,
    gb,
    grow,
    gown,
    goth,
    glr,
    hbuf,
    b2,
    adb,
    lsem,
    ssem,
    rsem,
    hsem,
):
    t, i, j = lax.axis_index("tm"), lax.axis_index("lat"), lax.axis_index("lon")
    ch = j // 2
    rg = j % 2

    def send(src, dst, phase, where):
        pltpu.make_async_remote_copy(
            src_ref=src,
            dst_ref=dst,
            send_sem=ssem.at[phase],
            recv_sem=rsem.at[phase],
            device_id=where,
            device_id_type=MESH,
        ).start()

    def arrived(ref, phase):
        pltpu.make_async_copy(ref, ref, rsem.at[phase]).wait()

    def sent(ref, phase):
        pltpu.make_async_copy(ref, ref, ssem.at[phase]).wait()

    def loop(first, last, body):
        for k in range(first, last):
            body(k)

    def around(start, step, size):
        return lax.rem(start + step, jnp.int32(size))

    def other_lats():
        if NL % 16:
            return [(k, None) for k in range(1, NL)]
        steps = []
        for u in (4, 3, 5, 2, 6, 1, 7, 0):
            steps += [(u, 1), (u, 0)]
        return steps[:-1]

    def lat_at(step):
        u, flip = step
        if flip is None:
            return around(i, u, NL)
        return around(i // 2, u, NL // 2) * 2 + around(i, flip, 2)

    lat_steps = other_lats()
    everywhere = [(step, k) for step in lat_steps for k in range(4)]
    everywhere += [(None, k) for k in (3, 2, 1)]

    def place_at(step_and_k):
        step, k = step_and_k
        return (i if step is None else lat_at(step)), around(j, k, 4)

    copies = [
        pltpu.make_async_copy(src, dst, lsem.at[n])
        for n, (src, dst) in enumerate(
            (
                (pert, pv),
                (ilat, vlat),
                (ilon, vlon),
                (o_cell, vcell),
                (o_count, vcount),
                (o_value, vvalue),
                (o_weight, vweight),
                (ctl.at[:, t], cs),
                (latf, lf),
                (lonf.at[pl.ds(ch * 256, 256)], nf),
            )
        )
    ]
    for copy in copies:
        copy.start()

    ready = pltpu.get_barrier_semaphore()

    def hello(*where):
        pl.semaphore_signal(ready, inc=1, device_id=where, device_id_type=MESH)

    for spot in everywhere:
        hello(t, *place_at(spot))
    loop(4, 4 * NT, lambda k: hello(around(t, k // 4, NT), i, around(j, k, 4)))

    @pl.when(i < NL - 1)
    def _():
        loop(2, 2 * NT, lambda k: hello(around(t, k // 2, NT), i + 1, (k % 2) * 2))

        @pl.when(rg == 1)
        def _():
            loop(2, 2 * NT, lambda k: hello(around(t, k // 2, NT), i + 1, (k % 2) * 2 + 1))

    @pl.when(i > 0)
    def _():
        loop(2, 2 * NT, lambda k: hello(around(t, k // 2, NT), i - 1, (k % 2) * 2 + 1))

        @pl.when(rg == 0)
        def _():
            loop(2, 2 * NT, lambda k: hello(around(t, k // 2, NT), i - 1, (k % 2) * 2))

    peers = 4 * NL - 1 + 4 * NT - 4
    peers = peers + jnp.where(i < NL - 1, (NT - 1) * (2 + 2 * rg), 0)
    peers = peers + jnp.where(i > 0, (NT - 1) * (4 - 2 * rg), 0)

    copies[0].wait()

    def widen(l):
        x = pv[:, l].astype(F32)
        psend[l * 2] = x[:, :8]
        psend[l * 2 + 1] = x[:, 8:]

    loop(0, NT, widen)
    for copy in copies[1:7]:
        copy.wait()
    opk[...] = jnp.zeros(opk.shape, F32)
    slot_entry = lax.broadcasted_iota(jnp.int32, (1, 64), 1)
    for s in range(NT):
        usable = slot_entry < vcount[0:1, s : s + 1]
        opk[s, 0:1, :64] = vcell[s].astype(F32)
        opk[s, 1:2, :64] = vvalue[s]
        opk[s, 2:3, :64] = jnp.where(usable, vweight[s], 0.0)

    @pl.when(i == 0)
    def _():
        lr[: 4 * NT] = jnp.zeros((4 * NT, 1, COLS), F32)

    @pl.when(i == NL - 1)
    def _():
        lr[4 * NT :] = jnp.zeros((4 * NT, 1, COLS), F32)

    no_rim = jnp.logical_or(
        jnp.logical_and(rg == 0, i == 0), jnp.logical_and(rg == 1, i == NL - 1)
    )
    rim = jnp.logical_not(no_rim)

    @pl.when(no_rim)
    def _():
        glr[...] = jnp.zeros(glr.shape, F32)

    wbuf[...] = jnp.zeros(wbuf.shape, F32)
    for copy in copies[7:]:
        copy.wait()
    lat_m = lf[...]
    lat_t = lat_m.astype(F32).T.astype(BF16)
    pl.semaphore_wait(ready, peers)

    for step in lat_steps:
        to = lat_at(step)
        send(cs.at[to], abuf.at[i], 0, (t, to, j))
    abuf[i] = cs[i]

    def send_o(k):
        to = around(t, k, NT)
        send(opk.at[to], obuf.at[t], 1, (to, i, j))

    loop(1, NT, send_o)
    obuf[t] = opk[t]

    def send_p(k):
        to = around(t, k // 2, NT)
        half = around(rg, k, 2)
        send(psend.at[to * 2 + half], pbuf.at[t * 2 + rg], 2, (to, i, ch * 2 + half))

    loop(1, 2 * NT, send_p)
    pbuf[t * 2 + rg] = psend[t * 2 + rg]

    k_row = lax.broadcasted_iota(jnp.int32, (KR, 18), 0)
    k_col = lax.broadcasted_iota(jnp.int32, (KR, 18), 1)
    inner = NT * 16
    place = jnp.where(
        k_row < inner,
        1 + (k_row & 15),
        jnp.where(k_row < inner + NT, 0, jnp.where(k_row < inner + 2 * NT, ROWS + 1, -1)),
    )
    pick = (place == k_col).astype(F32)
    p_rows = nn(pick, vlat[...], precision=HIGHEST)
    q_row = lax.broadcasted_iota(jnp.int32, (256, COLS + 2), 0)
    q_col = lax.broadcasted_iota(jnp.int32, (256, COLS + 2), 1)
    place = jnp.where(
        q_row < COLS, q_row + 1, jnp.where(q_row == 255, 0, jnp.where(q_row == COLS, COLS + 1, -1))
    )
    pick = (place == q_col).astype(F32)
    q_rows = nn(pick, vlon[...], precision=HIGHEST)
    arrived(obuf.at[pl.ds(0, NT - 1)], 1)
    lists = jnp.concatenate(
        [obuf[2 * k] + pltpu.roll(obuf[2 * k + 1], 64, 1) for k in range(NT // 2)], axis=1
    )
    n_obs = NT * 64
    cell = lists[0:1].astype(jnp.int32)
    target = lists[1:2]
    weight = lists[2:3]
    o_lev = cell >> 13
    o_row = (cell >> 8) & 31
    o_col = cell & 255
    hot_row = (lax.broadcasted_iota(jnp.int32, (FINE_ROWS, n_obs), 0) == o_row).astype(F32)
    hot_col = (lax.broadcasted_iota(jnp.int32, (FINE_COLS, n_obs), 0) == o_col).astype(F32)
    lev = lax.broadcasted_iota(jnp.int32, (KR, n_obs), 0)
    lev = jnp.where(lev < inner, lev >> 4, jnp.where(lev < inner + NT, lev - inner, lev - inner - NT))
    r_mat = nn(p_rows, hot_row, precision=HIGHEST)
    rtb[...] = jnp.where(lev == o_lev, r_mat, 0.0)
    ctb[...] = nn(q_rows, hot_col, precision=HIGHEST)

    arrived(abuf.at[pl.ds(0, NL - 1)], 0)
    high, low = halves(abuf[...].reshape(NL * ROWS, COLS))
    both = nn(lat_m, jnp.concatenate([high, low], axis=1))
    ybuf[...] = (both[:, :COLS] + both[:, COLS:]).reshape(2 * NL, 8, COLS)

    for spot in everywhere:
        lat, lon = place_at(spot)
        send(ybuf.at[lat * 2 + around(lon, 0, 2)], bbuf.at[j * NL + i], 3, (t, lat, lon))
    bbuf[j * NL + i] = ybuf[i * 2 + rg]
    arrived(bbuf.at[pl.ds(0, 4 * NL - 1)], 3)

    m8 = NL * 8
    wide = jnp.concatenate(
        [bbuf[NL * b : NL * b + NL].reshape(m8, COLS) for b in range(4)], axis=1
    )
    lon_m = nf[...]
    both = nt(jnp.concatenate(halves(wide), axis=0), lon_m)
    z = both[:m8] + both[m8:]
    z0 = z[:, :COLS].reshape(NL, 8, COLS)
    z1 = z[:, COLS:].reshape(NL, 8, COLS)

    arrived(pbuf.at[pl.ds(0, 2 * NT - 1)], 2)

    for s in range(NT):
        for blk, zz in enumerate((z0, z1)):
            x = jnp.sum(zz * pbuf[2 * s + blk], axis=0)
            inc[2 * s + blk] = x
            rows[2 * s + blk] = jnp.where(rg == 0, x[0:1], x[7:8])

    @pl.when(rim)
    def _():
        lat = i + 2 * rg - 1
        spot = ((1 - rg) * NT + t) * 4 + ch * 2

        def send_f(k):
            s = around(t, k // 4, NT)
            send(rows.at[pl.ds(2 * s, 2)], lr.at[pl.ds(spot, 2)], 6 + rg, (s, lat, k % 4))

        loop(0, 4 * NT, send_f)

    def send_e(k):
        s = around(t, k // 2, NT)
        e = k % 2
        send(inc.at[2 * s + 1 - e], woth.at[t * 2 + rg], 5, (s, i, 2 - 2 * ch + e))

    loop(0, 2 * NT, send_e)

    def send_d(k):
        s = around(t, k // 2, NT)
        lon = ch * 2 + around(rg, k, 2)
        send(inc.at[pl.ds(2 * s, 2)], wown.at[pl.ds((t * 2 + rg) * 2, 2)], 4, (s, i, lon))

    loop(1, 2 * NT, send_d)

    wown[(t * 2 + rg) * 2] = inc[2 * t]
    wown[(t * 2 + rg) * 2 + 1] = inc[2 * t + 1]

    arrived(wown.at[pl.ds(0, 2 * (2 * NT - 1))], 4)
    arrived(woth, 5)

    @pl.when(i > 0)
    def _():
        arrived(lr.at[pl.ds(0, 4 * NT)], 7)

    @pl.when(i < NL - 1)
    def _():
        arrived(lr.at[pl.ds(4 * NT, 4 * NT)], 6)

    even = rg == 0
    w = wown[...].reshape(2 * NT, 2, 8, COLS)
    w0, w1 = w[:, 0].reshape(16 * NT, COLS), w[:, 1].reshape(16 * NT, COLS)
    lane = lax.broadcasted_iota(jnp.int32, (16 * NT, COLS), 1)
    near = jnp.where(even, 0, COLS - 1)
    far = COLS - 1 - near
    wbuf[:inner, :COLS] = jnp.where(even, w0, w1)
    wbuf[:inner, COLS:] = jnp.where(
        lane == near,
        jnp.where(even, w1, w0),
        jnp.where(lane == far, woth[...].reshape(16 * NT, COLS), 0.0),
    )
    lane1 = lax.broadcasted_iota(jnp.int32, (1, COLS), 1)
    for k in range(2 * NT):
        before = lr[k * 4 + (j + 3) % 4]
        after = lr[k * 4 + (j + 1) % 4]
        wbuf[inner + k : inner + k + 1, :COLS] = lr[k * 4 + j]
        wbuf[inner + k : inner + k + 1, COLS:] = jnp.where(
            lane1 == COLS - 1, before, jnp.where(lane1 == 0, after, 0.0)
        )

    r_high, r_low = halves(rtb[...])
    w_high, w_low = halves(wbuf[...].T)
    both = nn(jnp.concatenate([w_high, w_low], axis=0), r_high)
    mixed = both[:256] + both[256:] + nn(w_high, r_low)
    cols = ctb[...]
    seen = jnp.sum(mixed * cols, axis=0, keepdims=True)
    departure = weight * (seen - target)
    d_high, d_low = halves(cols * departure)
    both = nt(jnp.concatenate([r_high, r_low], axis=0), d_high)
    g = both[:KR] + both[KR:] + nt(r_high, d_low)
    for k in range(2 * NT):
        gb[2 * k] = g[8 * k : 8 * k + 8, :COLS]
        gb[2 * k + 1] = g[8 * k : 8 * k + 8, COLS:]
    for k in range(2 * NT):
        grow[2 * k] = g[inner + k : inner + k + 1, :COLS]
        grow[2 * k + 1] = g[inner + k : inner + k + 1, COLS:]

    def send_rim(pos):
        def go(k):
            l = around(t, k // 2, NT)
            send(
                grow.at[pl.ds((pos * NT + l) * 2, 2)],
                glr.at[pl.ds((t * 4 + j) * 2, 2)],
                10 + pos,
                (l, i - 1 + 2 * pos, (k % 2) * 2 + 1 - pos),
            )

        loop(0, 2 * NT, go)

    @pl.when(i > 0)
    def _():
        send_rim(0)

    @pl.when(i < NL - 1)
    def _():
        send_rim(1)

    def send_h(k):
        l = around(t, k // 2, NT)
        half = k % 2
        send(
            gb.at[(l * 2 + half) * 2 + 1], goth.at[t * 2 + rg], 9, (l, i, 2 - 2 * ch + half)
        )

    loop(0, 2 * NT, send_h)

    def send_g(k):
        l = around(t, k // 2, NT)
        half = around(rg, k, 2)
        send(
            gb.at[pl.ds((l * 2 + half) * 2, 2)],
            gown.at[pl.ds((t * 2 + rg) * 2, 2)],
            8,
            (l, i, ch * 2 + half),
        )

    loop(1, 2 * NT, send_g)

    gown[(t * 2 + rg) * 2] = gb[(t * 2 + rg) * 2]
    gown[(t * 2 + rg) * 2 + 1] = gb[(t * 2 + rg) * 2 + 1]
    arrived(gown.at[pl.ds(0, 2 * (2 * NT - 1))], 8)
    arrived(goth, 9)

    @pl.when(jnp.logical_and(rim, rg == 1))
    def _():
        arrived(glr, 10)

    @pl.when(jnp.logical_and(rim, rg == 0))
    def _():
        arrived(glr, 11)

    lane8 = lax.broadcasted_iota(jnp.int32, (8, COLS), 1)
    row8 = lax.broadcasted_iota(jnp.int32, (8, COLS), 0)
    first, last = lane8 == 0, lane8 == COLS - 1
    mine = row8 == jnp.where(even, 0, 7)
    other = 2 - 2 * ch
    acc0 = acc1 = None
    for s in range(NT):
        def rim_of(b, part, s=s):
            return jnp.broadcast_to(glr[(s * 4 + b) * 2 + part], (8, COLS))

        d0 = gown[s * 4] + jnp.where(last, gown[s * 4 + 3], 0.0)
        d0 = d0 + jnp.where(first, goth[s * 2 + 1], 0.0)
        e0 = rim_of(ch * 2, 0) + jnp.where(last, rim_of(ch * 2 + 1, 1), 0.0)
        e0 = e0 + jnp.where(first, rim_of(other + 1, 1), 0.0)
        d0 = d0 + jnp.where(mine, e0, 0.0)
        d1 = gown[s * 4 + 2] + jnp.where(first, gown[s * 4 + 1], 0.0)
        d1 = d1 + jnp.where(last, goth[s * 2], 0.0)
        e1 = rim_of(ch * 2 + 1, 0) + jnp.where(first, rim_of(ch * 2, 1), 0.0)
        e1 = e1 + jnp.where(last, rim_of(other, 1), 0.0)
        d1 = d1 + jnp.where(mine, e1, 0.0)
        p0, p1 = pbuf[2 * s] * d0[None], pbuf[2 * s + 1] * d1[None]
        acc0, acc1 = (p0, p1) if s == 0 else (acc0 + p0, acc1 + p1)
    grad = jnp.concatenate([acc0.reshape(m8, COLS), acc1.reshape(m8, COLS)], axis=1)
    both = nn(jnp.concatenate(halves(grad), axis=0), lon_m)
    h = both[:m8] + both[m8:]
    for b in range(4):
        hbuf[NL * b : NL * b + NL] = h[:, b * COLS : (b + 1) * COLS].reshape(NL, 8, COLS)

    for spot in everywhere:
        lat, lon = place_at(spot)
        send(hbuf.at[lon * NL + lat], b2.at[ch * 2 * NL + 2 * i + rg], 12, (t, lat, lon))

    b2[ch * 2 * NL + 2 * i + rg] = hbuf[j * NL + i]
    arrived(b2.at[pl.ds(0, 4 * NL - 1)], 12)
    y = (b2[: 2 * NL] + b2[2 * NL :]).reshape(NL * ROWS, COLS)
    high, low = halves(y)
    both = nn(lat_t, jnp.concatenate([high, low], axis=1))
    adb[...] = (both[:, :COLS] + both[:, COLS:]).reshape(NL, ROWS, COLS)

    chunks = 4 if NL % 4 == 0 else NL
    size = NL // chunks
    own = i // size

    for step in lat_steps:
        to = lat_at(step)
        send(adb.at[to], out.at[i, t], 16 + own, (t, to, j))

    out[i, t] = adb[i]

    core = t % 2
    sibling = t + 1 - 2 * core
    right, left = (t + 2) % NT, (t + NT - 2) % NT
    chips = NT // 2
    order = (0, 1, 3, 2) if chunks == 4 else tuple(range(chunks))
    places = [(own + o) % chunks for o in order]

    def chunk(q, owner):
        return out.at[pl.ds(q * size, size), owner]

    def pass_on(q, owner, n, to):
        pltpu.make_async_remote_copy(
            src_ref=chunk(q, owner),
            dst_ref=chunk(q, owner),
            send_sem=ssem.at[14],
            recv_sem=hsem.at[n],
            device_id=(to, i, j),
            device_id_type=MESH,
        ).start()

    def landed(q, n):
        pltpu.make_async_copy(chunk(q, t), chunk(q, t), hsem.at[n]).wait()

    from_left, from_right, from_far, from_sibling = 0, chunks, 2 * chunks, 3 * chunks

    def relay(k):
        q = places[k]
        landed(q, from_left + k)
        if 2 * k < chunks:
            pass_on(q, left, from_far + k, right)
        pass_on(q, left, from_sibling, sibling)
        landed(q, from_right + k)
        if 2 * k >= chunks:
            pass_on(q, right, from_far + k, left)
        pass_on(q, right, from_sibling, sibling)

    for k, q in enumerate(places):
        if k == 0:
            if size > 1:
                arrived(out.at[pl.ds(0, size - 1), t], 16 + q)
        else:
            arrived(out.at[pl.ds(0, size), t], 16 + q)
        if chips > 1:
            pass_on(q, t, from_left + k, right)
            pass_on(q, t, from_right + k, left)
        pass_on(q, t, from_sibling, sibling)
        if chips > 1 and k > 0:
            relay(k - 1)
    if chips > 1:
        relay(chunks - 1)
        across = (t + NT // 2) % NT
        for k, q in enumerate(places):
            landed(q, from_far + k)
            pass_on(q, across, from_sibling, sibling)
    everything = out.at[:, pl.ds(0, chips)]
    pltpu.make_async_copy(everything, everything, hsem.at[from_sibling]).wait()

    sent(abuf.at[pl.ds(0, NL - 1)], 0)
    sent(obuf.at[pl.ds(0, NT - 1)], 1)
    sent(pbuf.at[pl.ds(0, 2 * NT - 1)], 2)
    sent(bbuf.at[pl.ds(0, 4 * NL - 1)], 3)
    sent(wown.at[pl.ds(0, 2 * (2 * NT - 1))], 4)
    sent(woth, 5)

    @pl.when(jnp.logical_and(rim, rg == 0))
    def _():
        sent(glr, 6)

    @pl.when(jnp.logical_and(rim, rg == 1))
    def _():
        sent(glr, 7)

    sent(gown.at[pl.ds(0, 2 * (2 * NT - 1))], 8)
    sent(goth, 9)

    @pl.when(i > 0)
    def _():
        sent(lr.at[pl.ds(0, 4 * NT)], 10)

    @pl.when(i < NL - 1)
    def _():
        sent(lr.at[pl.ds(0, 4 * NT)], 11)

    sent(b2.at[pl.ds(0, 4 * NL - 1)], 12)
    sent(out.at[pl.ds(0, NL - 1), t], 16 + own)
    sent(out.at[:, pl.ds(0, NT - 1)], 14)


def per_device(NT, NL, control, pert, latf, lonf, ilat, ilon, cell, count, value, weight):
    hbm = pl.BlockSpec(memory_space=pltpu.HBM)
    V = pltpu.VMEM
    tile = (8, COLS)
    cap = cell.shape[-1]
    scratch = [
        V((ROWS + 2, FINE_ROWS), F32),
        V((COLS + 2, FINE_COLS), F32),
        V((NT, 1, cap), jnp.int32),
        V((1, NT), jnp.int32),
        V((NT, 1, cap), F32),
        V((NT, 1, cap), F32),
        V((NT, *tile), F32),
        V((NL, ROWS, COLS), F32),
        V((NL, NT, ROWS, COLS), BF16),
        V((NL * ROWS, NL * ROWS), BF16),
        V((256, 512), BF16),
        V((NL, ROWS, COLS), F32),
        V((NT, *tile), F32),
        V((2 * NT, NL, *tile), F32),
        V((2 * NT, NL, *tile), F32),
        V((2 * NL, *tile), F32),
        V((4 * NL, *tile), F32),
        V((2 * NT, *tile), F32),
        V((2 * NT, 1, COLS), F32),
        V((4 * NT, *tile), F32),
        V((2 * NT, *tile), F32),
        V((8 * NT, 1, COLS), F32),
        V((KR, 256), F32),
        V((KR, NT * 64), F32),
        V((256, NT * 64), F32),
        V((4 * NT, *tile), F32),
        V((4 * NT, 1, COLS), F32),
        V((4 * NT, *tile), F32),
        V((2 * NT, *tile), F32),
        V((8 * NT, 1, COLS), F32),
        V((4 * NL, *tile), F32),
        V((4 * NL, *tile), F32),
        V((NL, ROWS, COLS), F32),
        pltpu.SemaphoreType.DMA((10,)),
        pltpu.SemaphoreType.DMA((20,)),
        pltpu.SemaphoreType.DMA((20,)),
        pltpu.SemaphoreType.DMA((13,)),
    ]
    adjoint = pl.pallas_call(
        functools.partial(kernel, NT, NL),
        name="gradient",
        out_shape=jax.ShapeDtypeStruct(control.shape, F32),
        in_specs=[hbm] * 10,
        out_specs=pl.BlockSpec(memory_space=pltpu.VMEM),
        scratch_shapes=scratch,
        compiler_params=pltpu.CompilerParams(
            has_side_effects=True, collective_id=0, vmem_limit_bytes=63 * 1024 * 1024
        ),
    )(
        control,
        pert[0],
        latf,
        lonf,
        ilat.T,
        ilon.T,
        cell.reshape(NT, 1, cap),
        count.reshape(1, NT),
        value.reshape(NT, 1, cap),
        weight.reshape(NT, 1, cap),
    )
    return control + adjoint


def solution(mesh):
    placed = (
        P(None, None, "lat", "lon"),
        P("tm", None, None, "lat", "lon"),
        P(),
        P(),
        P("lat", None),
        P("lon", None),
        P("tm", None, "lat", "lon", None),
        P("tm", None, "lat", "lon"),
        P("tm", None, "lat", "lon", None),
        P("tm", None, "lat", "lon", None),
    )
    return jax.shard_map(
        functools.partial(per_device, mesh.shape["tm"], mesh.shape["lat"]),
        mesh=mesh,
        in_specs=placed,
        out_specs=P(None, None, "lat", "lon"),
        check_vma=False,
    )
```

```python
import functools

import jax
import jax.numpy as jnp
from jax import lax
from jax.experimental import pallas as pl
from jax.experimental.pallas import tpu as pltpu
from jax.sharding import PartitionSpec as P

F32 = jnp.float32
BF16 = jnp.bfloat16
HIGHEST = lax.Precision.HIGHEST
MESH = pl.DeviceIdType.MESH
ROWS, COLS = 16, 128
FINE_ROWS, FINE_COLS = 32, 256
KR = 256


def halves(x):
    high = x.astype(BF16)
    return high, (x - high.astype(F32)).astype(BF16)


def nt(a, b, **kw):
    return lax.dot_general(a, b, (((1,), (1,)), ((), ())), preferred_element_type=F32, **kw)


def nn(a, b, **kw):
    return lax.dot_general(a, b, (((1,), (0,)), ((), ())), preferred_element_type=F32, **kw)


def kernel(
    NT,
    NL,
    ctl,
    pert,
    latf,
    lonf,
    ilat,
    ilon,
    o_cell,
    o_count,
    o_value,
    o_weight,
    out,
    vlat,
    vlon,
    vcell,
    vcount,
    vvalue,
    vweight,
    opk,
    cs,
    pv,
    lf,
    nf,
    abuf,
    obuf,
    psend,
    pbuf,
    ybuf,
    bbuf,
    inc,
    rows,
    wown,
    woth,
    lr,
    wbuf,
    rtb,
    ctb,
    gb,
    grow,
    gown,
    goth,
    glr,
    hbuf,
    b2,
    adb,
    gat,
    lsem,
    ssem,
    rsem,
    hsem,
):
    t, i, j = lax.axis_index("tm"), lax.axis_index("lat"), lax.axis_index("lon")
    ch = j // 2
    rg = j % 2

    def send(src, dst, phase, where):
        pltpu.make_async_remote_copy(
            src_ref=src,
            dst_ref=dst,
            send_sem=ssem.at[phase],
            recv_sem=rsem.at[phase],
            device_id=where,
            device_id_type=MESH,
        ).start()

    def arrived(ref, phase):
        pltpu.make_async_copy(ref, ref, rsem.at[phase]).wait()

    def sent(ref, phase):
        pltpu.make_async_copy(ref, ref, ssem.at[phase]).wait()

    def loop(first, last, body):
        for k in range(first, last):
            body(k)

    def around(start, step, size):
        return lax.rem(start + step, jnp.int32(size))

    def other_lats():
        if NL % 16:
            return [(k, None) for k in range(1, NL)]
        steps = []
        for u in (4, 3, 5, 2, 6, 1, 7, 0):
            steps += [(u, 1), (u, 0)]
        return steps[:-1]

    def lat_at(step):
        u, flip = step
        if flip is None:
            return around(i, u, NL)
        return around(i // 2, u, NL // 2) * 2 + around(i, flip, 2)

    lat_steps = other_lats()
    everywhere = [(step, k) for step in lat_steps for k in range(4)]
    everywhere += [(None, k) for k in (3, 2, 1)]

    def place_at(step_and_k):
        step, k = step_and_k
        return (i if step is None else lat_at(step)), around(j, k, 4)

    copies = [
        pltpu.make_async_copy(src, dst, lsem.at[n])
        for n, (src, dst) in enumerate(
            (
                (pert, pv),
                (ilat, vlat),
                (ilon, vlon),
                (o_cell, vcell),
                (o_count, vcount),
                (o_value, vvalue),
                (o_weight, vweight),
                (ctl.at[:, t], cs),
                (latf, lf),
                (lonf.at[pl.ds(ch * 256, 256)], nf),
            )
        )
    ]
    for copy in copies:
        copy.start()

    ready = pltpu.get_barrier_semaphore()

    def hello(*where):
        pl.semaphore_signal(ready, inc=1, device_id=where, device_id_type=MESH)

    for spot in everywhere:
        hello(t, *place_at(spot))
    loop(4, 4 * NT, lambda k: hello(around(t, k // 4, NT), i, around(j, k, 4)))

    @pl.when(i < NL - 1)
    def _():
        loop(2, 2 * NT, lambda k: hello(around(t, k // 2, NT), i + 1, (k % 2) * 2))

        @pl.when(rg == 1)
        def _():
            loop(2, 2 * NT, lambda k: hello(around(t, k // 2, NT), i + 1, (k % 2) * 2 + 1))

    @pl.when(i > 0)
    def _():
        loop(2, 2 * NT, lambda k: hello(around(t, k // 2, NT), i - 1, (k % 2) * 2 + 1))

        @pl.when(rg == 0)
        def _():
            loop(2, 2 * NT, lambda k: hello(around(t, k // 2, NT), i - 1, (k % 2) * 2))

    peers = 4 * NL - 1 + 4 * NT - 4
    peers = peers + jnp.where(i < NL - 1, (NT - 1) * (2 + 2 * rg), 0)
    peers = peers + jnp.where(i > 0, (NT - 1) * (4 - 2 * rg), 0)

    copies[0].wait()

    def widen(l):
        x = pv[:, l].astype(F32)
        psend[l * 2] = x[:, :8]
        psend[l * 2 + 1] = x[:, 8:]

    loop(0, NT, widen)
    for copy in copies[1:7]:
        copy.wait()
    opk[...] = jnp.zeros(opk.shape, F32)
    slot_entry = lax.broadcasted_iota(jnp.int32, (1, 64), 1)
    for s in range(NT):
        usable = slot_entry < vcount[0:1, s : s + 1]
        opk[s, 0:1, :64] = vcell[s].astype(F32)
        opk[s, 1:2, :64] = vvalue[s]
        opk[s, 2:3, :64] = jnp.where(usable, vweight[s], 0.0)

    @pl.when(i == 0)
    def _():
        lr[: 4 * NT] = jnp.zeros((4 * NT, 1, COLS), F32)

    @pl.when(i == NL - 1)
    def _():
        lr[4 * NT :] = jnp.zeros((4 * NT, 1, COLS), F32)

    no_rim = jnp.logical_or(
        jnp.logical_and(rg == 0, i == 0), jnp.logical_and(rg == 1, i == NL - 1)
    )
    rim = jnp.logical_not(no_rim)

    @pl.when(no_rim)
    def _():
        glr[...] = jnp.zeros(glr.shape, F32)

    wbuf[...] = jnp.zeros(wbuf.shape, F32)
    for copy in copies[7:]:
        copy.wait()
    lat_m = lf[...]
    lat_t = lat_m.astype(F32).T.astype(BF16)
    pl.semaphore_wait(ready, peers)

    for step in lat_steps:
        to = lat_at(step)
        send(cs.at[to], abuf.at[i], 0, (t, to, j))
    abuf[i] = cs[i]

    def send_o(k):
        to = around(t, k, NT)
        send(opk.at[to], obuf.at[t], 1, (to, i, j))

    loop(1, NT, send_o)
    obuf[t] = opk[t]

    def send_p(k):
        to = around(t, k // 2, NT)
        half = around(rg, k, 2)
        send(psend.at[to * 2 + half], pbuf.at[t * 2 + rg], 2, (to, i, ch * 2 + half))

    loop(1, 2 * NT, send_p)
    pbuf[t * 2 + rg] = psend[t * 2 + rg]

    k_row = lax.broadcasted_iota(jnp.int32, (KR, 18), 0)
    k_col = lax.broadcasted_iota(jnp.int32, (KR, 18), 1)
    inner = NT * 16
    place = jnp.where(
        k_row < inner,
        1 + (k_row & 15),
        jnp.where(k_row < inner + NT, 0, jnp.where(k_row < inner + 2 * NT, ROWS + 1, -1)),
    )
    pick = (place == k_col).astype(F32)
    p_rows = nn(pick, vlat[...], precision=HIGHEST)
    q_row = lax.broadcasted_iota(jnp.int32, (256, COLS + 2), 0)
    q_col = lax.broadcasted_iota(jnp.int32, (256, COLS + 2), 1)
    place = jnp.where(
        q_row < COLS, q_row + 1, jnp.where(q_row == 255, 0, jnp.where(q_row == COLS, COLS + 1, -1))
    )
    pick = (place == q_col).astype(F32)
    q_rows = nn(pick, vlon[...], precision=HIGHEST)
    arrived(obuf.at[pl.ds(0, NT - 1)], 1)
    lists = jnp.concatenate(
        [obuf[2 * k] + pltpu.roll(obuf[2 * k + 1], 64, 1) for k in range(NT // 2)], axis=1
    )
    n_obs = NT * 64
    cell = lists[0:1].astype(jnp.int32)
    target = lists[1:2]
    weight = lists[2:3]
    o_lev = cell >> 13
    o_row = (cell >> 8) & 31
    o_col = cell & 255
    hot_row = (lax.broadcasted_iota(jnp.int32, (FINE_ROWS, n_obs), 0) == o_row).astype(F32)
    hot_col = (lax.broadcasted_iota(jnp.int32, (FINE_COLS, n_obs), 0) == o_col).astype(F32)
    lev = lax.broadcasted_iota(jnp.int32, (KR, n_obs), 0)
    lev = jnp.where(lev < inner, lev >> 4, jnp.where(lev < inner + NT, lev - inner, lev - inner - NT))
    r_mat = nn(p_rows, hot_row, precision=HIGHEST)
    rtb[...] = jnp.where(lev == o_lev, r_mat, 0.0)
    ctb[...] = nn(q_rows, hot_col, precision=HIGHEST)

    arrived(abuf.at[pl.ds(0, NL - 1)], 0)
    high, low = halves(abuf[...].reshape(NL * ROWS, COLS))
    both = nn(lat_m, jnp.concatenate([high, low], axis=1))
    ybuf[...] = (both[:, :COLS] + both[:, COLS:]).reshape(2 * NL, 8, COLS)

    for spot in everywhere:
        lat, lon = place_at(spot)
        send(ybuf.at[lat * 2 + around(lon, 0, 2)], bbuf.at[j * NL + i], 3, (t, lat, lon))
    bbuf[j * NL + i] = ybuf[i * 2 + rg]
    arrived(bbuf.at[pl.ds(0, 4 * NL - 1)], 3)

    m8 = NL * 8
    wide = jnp.concatenate(
        [bbuf[NL * b : NL * b + NL].reshape(m8, COLS) for b in range(4)], axis=1
    )
    lon_m = nf[...]
    both = nt(jnp.concatenate(halves(wide), axis=0), lon_m)
    z = both[:m8] + both[m8:]
    z0 = z[:, :COLS].reshape(NL, 8, COLS)
    z1 = z[:, COLS:].reshape(NL, 8, COLS)

    arrived(pbuf.at[pl.ds(0, 2 * NT - 1)], 2)

    for s in range(NT):
        for blk, zz in enumerate((z0, z1)):
            x = jnp.sum(zz * pbuf[2 * s + blk], axis=0)
            inc[2 * s + blk] = x
            rows[2 * s + blk] = jnp.where(rg == 0, x[0:1], x[7:8])

    @pl.when(rim)
    def _():
        lat = i + 2 * rg - 1
        spot = ((1 - rg) * NT + t) * 4 + ch * 2

        def send_f(k):
            s = around(t, k // 4, NT)
            send(rows.at[pl.ds(2 * s, 2)], lr.at[pl.ds(spot, 2)], 6 + rg, (s, lat, k % 4))

        loop(0, 4 * NT, send_f)

    def send_e(k):
        s = around(t, k // 2, NT)
        e = k % 2
        send(inc.at[2 * s + 1 - e], woth.at[t * 2 + rg], 5, (s, i, 2 - 2 * ch + e))

    loop(0, 2 * NT, send_e)

    def send_d(k):
        s = around(t, k // 2, NT)
        lon = ch * 2 + around(rg, k, 2)
        send(inc.at[pl.ds(2 * s, 2)], wown.at[pl.ds((t * 2 + rg) * 2, 2)], 4, (s, i, lon))

    loop(1, 2 * NT, send_d)

    wown[(t * 2 + rg) * 2] = inc[2 * t]
    wown[(t * 2 + rg) * 2 + 1] = inc[2 * t + 1]

    arrived(wown.at[pl.ds(0, 2 * (2 * NT - 1))], 4)
    arrived(woth, 5)

    @pl.when(i > 0)
    def _():
        arrived(lr.at[pl.ds(0, 4 * NT)], 7)

    @pl.when(i < NL - 1)
    def _():
        arrived(lr.at[pl.ds(4 * NT, 4 * NT)], 6)

    even = rg == 0
    w = wown[...].reshape(2 * NT, 2, 8, COLS)
    w0, w1 = w[:, 0].reshape(16 * NT, COLS), w[:, 1].reshape(16 * NT, COLS)
    lane = lax.broadcasted_iota(jnp.int32, (16 * NT, COLS), 1)
    near = jnp.where(even, 0, COLS - 1)
    far = COLS - 1 - near
    wbuf[:inner, :COLS] = jnp.where(even, w0, w1)
    wbuf[:inner, COLS:] = jnp.where(
        lane == near,
        jnp.where(even, w1, w0),
        jnp.where(lane == far, woth[...].reshape(16 * NT, COLS), 0.0),
    )
    lane1 = lax.broadcasted_iota(jnp.int32, (1, COLS), 1)
    for k in range(2 * NT):
        before = lr[k * 4 + (j + 3) % 4]
        after = lr[k * 4 + (j + 1) % 4]
        wbuf[inner + k : inner + k + 1, :COLS] = lr[k * 4 + j]
        wbuf[inner + k : inner + k + 1, COLS:] = jnp.where(
            lane1 == COLS - 1, before, jnp.where(lane1 == 0, after, 0.0)
        )

    r_high, r_low = halves(rtb[...])
    w_high, w_low = halves(wbuf[...].T)
    both = nn(jnp.concatenate([w_high, w_low], axis=0), r_high)
    mixed = both[:256] + both[256:] + nn(w_high, r_low)
    cols = ctb[...]
    seen = jnp.sum(mixed * cols, axis=0, keepdims=True)
    departure = weight * (seen - target)
    d_high, d_low = halves(cols * departure)
    both = nt(jnp.concatenate([r_high, r_low], axis=0), d_high)
    g = both[:KR] + both[KR:] + nt(r_high, d_low)
    for k in range(2 * NT):
        gb[2 * k] = g[8 * k : 8 * k + 8, :COLS]
        gb[2 * k + 1] = g[8 * k : 8 * k + 8, COLS:]
    for k in range(2 * NT):
        grow[2 * k] = g[inner + k : inner + k + 1, :COLS]
        grow[2 * k + 1] = g[inner + k : inner + k + 1, COLS:]

    def send_rim(pos):
        def go(k):
            l = around(t, k // 2, NT)
            send(
                grow.at[pl.ds((pos * NT + l) * 2, 2)],
                glr.at[pl.ds((t * 4 + j) * 2, 2)],
                10 + pos,
                (l, i - 1 + 2 * pos, (k % 2) * 2 + 1 - pos),
            )

        loop(0, 2 * NT, go)

    @pl.when(i > 0)
    def _():
        send_rim(0)

    @pl.when(i < NL - 1)
    def _():
        send_rim(1)

    def send_h(k):
        l = around(t, k // 2, NT)
        half = k % 2
        send(
            gb.at[(l * 2 + half) * 2 + 1], goth.at[t * 2 + rg], 9, (l, i, 2 - 2 * ch + half)
        )

    loop(0, 2 * NT, send_h)

    def send_g(k):
        l = around(t, k // 2, NT)
        half = around(rg, k, 2)
        send(
            gb.at[pl.ds((l * 2 + half) * 2, 2)],
            gown.at[pl.ds((t * 2 + rg) * 2, 2)],
            8,
            (l, i, ch * 2 + half),
        )

    loop(1, 2 * NT, send_g)

    gown[(t * 2 + rg) * 2] = gb[(t * 2 + rg) * 2]
    gown[(t * 2 + rg) * 2 + 1] = gb[(t * 2 + rg) * 2 + 1]
    arrived(gown.at[pl.ds(0, 2 * (2 * NT - 1))], 8)
    arrived(goth, 9)

    @pl.when(jnp.logical_and(rim, rg == 1))
    def _():
        arrived(glr, 10)

    @pl.when(jnp.logical_and(rim, rg == 0))
    def _():
        arrived(glr, 11)

    lane8 = lax.broadcasted_iota(jnp.int32, (8, COLS), 1)
    row8 = lax.broadcasted_iota(jnp.int32, (8, COLS), 0)
    first, last = lane8 == 0, lane8 == COLS - 1
    mine = row8 == jnp.where(even, 0, 7)
    other = 2 - 2 * ch
    acc0 = acc1 = None
    for s in range(NT):
        def rim_of(b, part, s=s):
            return jnp.broadcast_to(glr[(s * 4 + b) * 2 + part], (8, COLS))

        d0 = gown[s * 4] + jnp.where(last, gown[s * 4 + 3], 0.0)
        d0 = d0 + jnp.where(first, goth[s * 2 + 1], 0.0)
        e0 = rim_of(ch * 2, 0) + jnp.where(last, rim_of(ch * 2 + 1, 1), 0.0)
        e0 = e0 + jnp.where(first, rim_of(other + 1, 1), 0.0)
        d0 = d0 + jnp.where(mine, e0, 0.0)
        d1 = gown[s * 4 + 2] + jnp.where(first, gown[s * 4 + 1], 0.0)
        d1 = d1 + jnp.where(last, goth[s * 2], 0.0)
        e1 = rim_of(ch * 2 + 1, 0) + jnp.where(first, rim_of(ch * 2, 1), 0.0)
        e1 = e1 + jnp.where(last, rim_of(other, 1), 0.0)
        d1 = d1 + jnp.where(mine, e1, 0.0)
        p0, p1 = pbuf[2 * s] * d0[None], pbuf[2 * s + 1] * d1[None]
        acc0, acc1 = (p0, p1) if s == 0 else (acc0 + p0, acc1 + p1)
    grad = jnp.concatenate([acc0.reshape(m8, COLS), acc1.reshape(m8, COLS)], axis=1)
    both = nn(jnp.concatenate(halves(grad), axis=0), lon_m)
    h = both[:m8] + both[m8:]
    for b in range(4):
        hbuf[NL * b : NL * b + NL] = h[:, b * COLS : (b + 1) * COLS].reshape(NL, 8, COLS)

    for spot in everywhere:
        lat, lon = place_at(spot)
        send(hbuf.at[lon * NL + lat], b2.at[ch * 2 * NL + 2 * i + rg], 12, (t, lat, lon))

    b2[ch * 2 * NL + 2 * i + rg] = hbuf[j * NL + i]
    arrived(b2.at[pl.ds(0, 4 * NL - 1)], 12)
    y = (b2[: 2 * NL] + b2[2 * NL :]).reshape(NL * ROWS, COLS)
    high, low = halves(y)
    both = nn(lat_t, jnp.concatenate([high, low], axis=1))
    adb[...] = (both[:, :COLS] + both[:, COLS:]).reshape(NL, ROWS, COLS)

    for step in lat_steps:
        to = lat_at(step)
        send(adb.at[to], gat.at[i, t], 13, (t, to, j))

    gat[i, t] = adb[i]

    chunks = 4 if NL % 4 == 0 else NL
    size = NL // chunks
    half = chunks // 2
    chips = NT // 2
    core = lax.rem(t, jnp.int32(2))
    sibling = t + 1 - 2 * core
    right, left = around(t, 2, NT), around(t, NT - 2, NT)
    across = around(t, NT // 2, NT)

    def chunk(c, owner):
        return gat.at[pl.ds(c * size, size), owner]

    def pass_on(ref, n, to):
        pltpu.make_async_remote_copy(
            src_ref=ref,
            dst_ref=ref,
            send_sem=ssem.at[14],
            recv_sem=hsem.at[n],
            device_id=(to, i, j),
            device_id_type=MESH,
        ).start()

    def landed(c, n):
        pltpu.make_async_copy(chunk(c, t), chunk(c, t), hsem.at[n]).wait()

    outward = []

    def to_out(owner):
        n = len(outward)
        outward.append(pltpu.make_async_copy(gat.at[:, owner], out.at[:, owner], lsem.at[n]))
        outward[-1].start()

    from_left, from_right, from_far, from_sibling = 0, chunks, 2 * chunks, 3 * chunks
    rightward = list(range(chunks))
    leftward = rightward[half:] + rightward[:half]
    arrived(gat.at[pl.ds(0, NL - 1), t], 13)
    if chips > 1:
        for c, d in zip(rightward, leftward):
            pass_on(chunk(c, t), from_left + c, right)
            pass_on(chunk(d, t), from_right + d, left)
    pass_on(gat.at[:, t], from_sibling, sibling)
    to_out(t)
    if chips > 1:
        for c, d in zip(rightward, leftward):
            landed(c, from_left + c)
            if c < half:
                pass_on(chunk(c, left), from_far + c, right)
            pass_on(chunk(c, left), from_sibling, sibling)
            landed(d, from_right + d)
            if d >= half:
                pass_on(chunk(d, right), from_far + d, left)
            pass_on(chunk(d, right), from_sibling, sibling)
        to_out(left)
        to_out(right)
        for n in range(chunks):
            c = n // 2 + (n % 2) * half if chunks % 2 == 0 else n
            landed(c, from_far + c)
            pass_on(chunk(c, across), from_sibling, sibling)
        to_out(across)
    everything = gat.at[:, pl.ds(0, chips)]
    pltpu.make_async_copy(everything, everything, hsem.at[from_sibling]).wait()
    for chip in range(chips):
        to_out(2 * chip + 1 - core)

    sent(abuf.at[pl.ds(0, NL - 1)], 0)
    sent(obuf.at[pl.ds(0, NT - 1)], 1)
    sent(pbuf.at[pl.ds(0, 2 * NT - 1)], 2)
    sent(bbuf.at[pl.ds(0, 4 * NL - 1)], 3)
    sent(wown.at[pl.ds(0, 2 * (2 * NT - 1))], 4)
    sent(woth, 5)

    @pl.when(jnp.logical_and(rim, rg == 0))
    def _():
        sent(glr, 6)

    @pl.when(jnp.logical_and(rim, rg == 1))
    def _():
        sent(glr, 7)

    sent(gown.at[pl.ds(0, 2 * (2 * NT - 1))], 8)
    sent(goth, 9)

    @pl.when(i > 0)
    def _():
        sent(lr.at[pl.ds(0, 4 * NT)], 10)

    @pl.when(i < NL - 1)
    def _():
        sent(lr.at[pl.ds(0, 4 * NT)], 11)

    sent(b2.at[pl.ds(0, 4 * NL - 1)], 12)
    sent(gat.at[pl.ds(0, NL - 1), t], 13)
    sent(gat.at[:, pl.ds(0, NT - 1)], 14)
    for copy in outward:
        copy.wait()


def per_device(NT, NL, control, pert, latf, lonf, ilat, ilon, cell, count, value, weight):
    hbm = pl.BlockSpec(memory_space=pltpu.HBM)
    V = pltpu.VMEM
    tile = (8, COLS)
    cap = cell.shape[-1]
    scratch = [
        V((ROWS + 2, FINE_ROWS), F32),
        V((COLS + 2, FINE_COLS), F32),
        V((NT, 1, cap), jnp.int32),
        V((1, NT), jnp.int32),
        V((NT, 1, cap), F32),
        V((NT, 1, cap), F32),
        V((NT, *tile), F32),
        V((NL, ROWS, COLS), F32),
        V((NL, NT, ROWS, COLS), BF16),
        V((NL * ROWS, NL * ROWS), BF16),
        V((256, 512), BF16),
        V((NL, ROWS, COLS), F32),
        V((NT, *tile), F32),
        V((2 * NT, NL, *tile), F32),
        V((2 * NT, NL, *tile), F32),
        V((2 * NL, *tile), F32),
        V((4 * NL, *tile), F32),
        V((2 * NT, *tile), F32),
        V((2 * NT, 1, COLS), F32),
        V((4 * NT, *tile), F32),
        V((2 * NT, *tile), F32),
        V((8 * NT, 1, COLS), F32),
        V((KR, 256), F32),
        V((KR, NT * 64), F32),
        V((256, NT * 64), F32),
        V((4 * NT, *tile), F32),
        V((4 * NT, 1, COLS), F32),
        V((4 * NT, *tile), F32),
        V((2 * NT, *tile), F32),
        V((8 * NT, 1, COLS), F32),
        V((4 * NL, *tile), F32),
        V((4 * NL, *tile), F32),
        V((NL, ROWS, COLS), F32),
        V((NL, NT, ROWS, COLS), F32),
        pltpu.SemaphoreType.DMA((10,)),
        pltpu.SemaphoreType.DMA((15,)),
        pltpu.SemaphoreType.DMA((15,)),
        pltpu.SemaphoreType.DMA((13,)),
    ]
    adjoint = pl.pallas_call(
        functools.partial(kernel, NT, NL),
        name="gradient",
        out_shape=jax.ShapeDtypeStruct(control.shape, F32),
        in_specs=[hbm] * 10,
        out_specs=hbm,
        scratch_shapes=scratch,
        compiler_params=pltpu.CompilerParams(
            has_side_effects=True, collective_id=0, vmem_limit_bytes=63 * 1024 * 1024
        ),
    )(
        control,
        pert[0],
        latf,
        lonf,
        ilat.T,
        ilon.T,
        cell.reshape(NT, 1, cap),
        count.reshape(1, NT),
        value.reshape(NT, 1, cap),
        weight.reshape(NT, 1, cap),
    )
    return control + adjoint


def solution(mesh):
    placed = (
        P(None, None, "lat", "lon"),
        P("tm", None, None, "lat", "lon"),
        P(),
        P(),
        P("lat", None),
        P("lon", None),
        P("tm", None, "lat", "lon", None),
        P("tm", None, "lat", "lon"),
        P("tm", None, "lat", "lon", None),
        P("tm", None, "lat", "lon", None),
    )
    return jax.shard_map(
        functools.partial(per_device, mesh.shape["tm"], mesh.shape["lat"]),
        mesh=mesh,
        in_specs=placed,
        out_specs=P(None, None, "lat", "lon"),
        check_vma=False,
    )
```

```python
import functools

import jax
import jax.numpy as jnp
from jax import lax
from jax.experimental import pallas as pl
from jax.experimental.pallas import tpu as pltpu
from jax.sharding import PartitionSpec as P

F32 = jnp.float32
BF16 = jnp.bfloat16
HIGHEST = lax.Precision.HIGHEST
MESH = pl.DeviceIdType.MESH
ROWS, COLS = 16, 128
FINE_ROWS, FINE_COLS = 32, 256
KR = 256
HELD = 3


def halves(x):
    high = x.astype(BF16)
    return high, (x - high.astype(F32)).astype(BF16)


def nt(a, b, **kw):
    return lax.dot_general(a, b, (((1,), (1,)), ((), ())), preferred_element_type=F32, **kw)


def nn(a, b, **kw):
    return lax.dot_general(a, b, (((1,), (0,)), ((), ())), preferred_element_type=F32, **kw)


def kernel(
    NT,
    NL,
    ctl,
    pert,
    latf,
    lonf,
    ilat,
    ilon,
    o_cell,
    o_count,
    o_value,
    o_weight,
    out,
    vlat,
    vlon,
    vcell,
    vcount,
    vvalue,
    vweight,
    opk,
    cs,
    pv,
    lf,
    nf,
    abuf,
    obuf,
    psend,
    pbuf,
    ybuf,
    bbuf,
    inc,
    rows,
    wown,
    woth,
    lr,
    wbuf,
    rtb,
    ctb,
    gb,
    grow,
    gown,
    goth,
    glr,
    hbuf,
    b2,
    adb,
    gat,
    lsem,
    ssem,
    rsem,
    hsem,
):
    t, i, j = lax.axis_index("tm"), lax.axis_index("lat"), lax.axis_index("lon")
    ch = j // 2
    rg = j % 2

    def send(src, dst, phase, where):
        pltpu.make_async_remote_copy(
            src_ref=src,
            dst_ref=dst,
            send_sem=ssem.at[phase],
            recv_sem=rsem.at[phase],
            device_id=where,
            device_id_type=MESH,
        ).start()

    def arrived(ref, phase):
        pltpu.make_async_copy(ref, ref, rsem.at[phase]).wait()

    def sent(ref, phase):
        pltpu.make_async_copy(ref, ref, ssem.at[phase]).wait()

    def loop(first, last, body):
        for k in range(first, last):
            body(k)

    def around(start, step, size):
        return lax.rem(start + step, jnp.int32(size))

    def other_lats():
        if NL % 16:
            return [(k, None) for k in range(1, NL)]
        steps = []
        for u in (4, 3, 5, 2, 6, 1, 7, 0):
            steps += [(u, 1), (u, 0)]
        return steps[:-1]

    def lat_at(step):
        u, flip = step
        if flip is None:
            return around(i, u, NL)
        return around(i // 2, u, NL // 2) * 2 + around(i, flip, 2)

    lat_steps = other_lats()
    everywhere = [(step, k) for step in lat_steps for k in range(4)]
    everywhere += [(None, k) for k in (3, 2, 1)]

    def place_at(step_and_k):
        step, k = step_and_k
        return (i if step is None else lat_at(step)), around(j, k, 4)

    copies = [
        pltpu.make_async_copy(src, dst, lsem.at[n])
        for n, (src, dst) in enumerate(
            (
                (pert, pv),
                (ilat, vlat),
                (ilon, vlon),
                (o_cell, vcell),
                (o_count, vcount),
                (o_value, vvalue),
                (o_weight, vweight),
                (ctl.at[:, t], cs),
                (latf, lf),
                (lonf.at[pl.ds(ch * 256, 256)], nf),
            )
        )
    ]
    for copy in copies:
        copy.start()

    ready = pltpu.get_barrier_semaphore()

    def hello(*where):
        pl.semaphore_signal(ready, inc=1, device_id=where, device_id_type=MESH)

    for spot in everywhere:
        hello(t, *place_at(spot))
    loop(4, 4 * NT, lambda k: hello(around(t, k // 4, NT), i, around(j, k, 4)))

    @pl.when(i < NL - 1)
    def _():
        loop(2, 2 * NT, lambda k: hello(around(t, k // 2, NT), i + 1, (k % 2) * 2))

        @pl.when(rg == 1)
        def _():
            loop(2, 2 * NT, lambda k: hello(around(t, k // 2, NT), i + 1, (k % 2) * 2 + 1))

    @pl.when(i > 0)
    def _():
        loop(2, 2 * NT, lambda k: hello(around(t, k // 2, NT), i - 1, (k % 2) * 2 + 1))

        @pl.when(rg == 0)
        def _():
            loop(2, 2 * NT, lambda k: hello(around(t, k // 2, NT), i - 1, (k % 2) * 2))

    peers = 4 * NL - 1 + 4 * NT - 4
    peers = peers + jnp.where(i < NL - 1, (NT - 1) * (2 + 2 * rg), 0)
    peers = peers + jnp.where(i > 0, (NT - 1) * (4 - 2 * rg), 0)

    copies[0].wait()

    def widen(l):
        x = pv[:, l].astype(F32)
        psend[l * 2] = x[:, :8]
        psend[l * 2 + 1] = x[:, 8:]

    loop(0, NT, widen)
    for copy in copies[1:7]:
        copy.wait()
    opk[...] = jnp.zeros(opk.shape, F32)
    slot_entry = lax.broadcasted_iota(jnp.int32, (1, 64), 1)
    for s in range(NT):
        usable = slot_entry < vcount[0:1, s : s + 1]
        opk[s, 0:1, :64] = vcell[s].astype(F32)
        opk[s, 1:2, :64] = vvalue[s]
        opk[s, 2:3, :64] = jnp.where(usable, vweight[s], 0.0)

    @pl.when(i == 0)
    def _():
        lr[: 4 * NT] = jnp.zeros((4 * NT, 1, COLS), F32)

    @pl.when(i == NL - 1)
    def _():
        lr[4 * NT :] = jnp.zeros((4 * NT, 1, COLS), F32)

    no_rim = jnp.logical_or(
        jnp.logical_and(rg == 0, i == 0), jnp.logical_and(rg == 1, i == NL - 1)
    )
    rim = jnp.logical_not(no_rim)

    @pl.when(no_rim)
    def _():
        glr[...] = jnp.zeros(glr.shape, F32)

    wbuf[...] = jnp.zeros(wbuf.shape, F32)
    for copy in copies[7:]:
        copy.wait()
    lat_m = lf[...]
    lat_t = lat_m.astype(F32).T.astype(BF16)
    pl.semaphore_wait(ready, peers)

    for step in lat_steps:
        to = lat_at(step)
        send(cs.at[to], abuf.at[i], 0, (t, to, j))
    abuf[i] = cs[i]

    def send_o(k):
        to = around(t, k, NT)
        send(opk.at[to], obuf.at[t], 1, (to, i, j))

    loop(1, NT, send_o)
    obuf[t] = opk[t]

    def send_p(k):
        to = around(t, k // 2, NT)
        half = around(rg, k, 2)
        send(psend.at[to * 2 + half], pbuf.at[t * 2 + rg], 2, (to, i, ch * 2 + half))

    held = [2 * k + 1 for k in dict.fromkeys((0, NT - 1, 1, NT - 2, 2, NT - 3))][:HELD]
    for k in range(1, 2 * NT):
        if k not in held:
            send_p(k)
    pbuf[t * 2 + rg] = psend[t * 2 + rg]

    k_row = lax.broadcasted_iota(jnp.int32, (KR, 18), 0)
    k_col = lax.broadcasted_iota(jnp.int32, (KR, 18), 1)
    inner = NT * 16
    place = jnp.where(
        k_row < inner,
        1 + (k_row & 15),
        jnp.where(k_row < inner + NT, 0, jnp.where(k_row < inner + 2 * NT, ROWS + 1, -1)),
    )
    pick = (place == k_col).astype(F32)
    p_rows = nn(pick, vlat[...], precision=HIGHEST)
    q_row = lax.broadcasted_iota(jnp.int32, (256, COLS + 2), 0)
    q_col = lax.broadcasted_iota(jnp.int32, (256, COLS + 2), 1)
    place = jnp.where(
        q_row < COLS, q_row + 1, jnp.where(q_row == 255, 0, jnp.where(q_row == COLS, COLS + 1, -1))
    )
    pick = (place == q_col).astype(F32)
    q_rows = nn(pick, vlon[...], precision=HIGHEST)
    arrived(obuf.at[pl.ds(0, NT - 1)], 1)
    lists = jnp.concatenate(
        [obuf[2 * k] + pltpu.roll(obuf[2 * k + 1], 64, 1) for k in range(NT // 2)], axis=1
    )
    n_obs = NT * 64
    cell = lists[0:1].astype(jnp.int32)
    target = lists[1:2]
    weight = lists[2:3]
    o_lev = cell >> 13
    o_row = (cell >> 8) & 31
    o_col = cell & 255
    hot_row = (lax.broadcasted_iota(jnp.int32, (FINE_ROWS, n_obs), 0) == o_row).astype(F32)
    hot_col = (lax.broadcasted_iota(jnp.int32, (FINE_COLS, n_obs), 0) == o_col).astype(F32)
    lev = lax.broadcasted_iota(jnp.int32, (KR, n_obs), 0)
    lev = jnp.where(lev < inner, lev >> 4, jnp.where(lev < inner + NT, lev - inner, lev - inner - NT))
    r_mat = nn(p_rows, hot_row, precision=HIGHEST)
    high, low = halves(jnp.where(lev == o_lev, r_mat, 0.0))
    rtb[:KR] = high
    rtb[KR:] = low
    ctb[...] = nn(q_rows, hot_col, precision=HIGHEST)

    arrived(abuf.at[pl.ds(0, NL - 1)], 0)
    high, low = halves(abuf[...].reshape(NL * ROWS, COLS))
    both = nn(lat_m, jnp.concatenate([high, low], axis=1))
    ybuf[...] = (both[:, :COLS] + both[:, COLS:]).reshape(2 * NL, 8, COLS)

    for spot in everywhere:
        lat, lon = place_at(spot)
        send(ybuf.at[lat * 2 + around(lon, 0, 2)], bbuf.at[j * NL + i], 3, (t, lat, lon))
    for k in held:
        send_p(k)
    bbuf[j * NL + i] = ybuf[i * 2 + rg]
    arrived(bbuf.at[pl.ds(0, 4 * NL - 1)], 3)

    m8 = NL * 8
    wide = jnp.concatenate(
        [bbuf[NL * b : NL * b + NL].reshape(m8, COLS) for b in range(4)], axis=1
    )
    lon_m = nf[...]
    both = nt(jnp.concatenate(halves(wide), axis=0), lon_m)
    z = both[:m8] + both[m8:]
    z0 = z[:, :COLS].reshape(NL, 8, COLS)
    z1 = z[:, COLS:].reshape(NL, 8, COLS)

    arrived(pbuf.at[pl.ds(0, 2 * NT - 1)], 2)

    for s in range(NT):
        for blk, zz in enumerate((z0, z1)):
            x = jnp.sum(zz * pbuf[2 * s + blk], axis=0)
            inc[2 * s + blk] = x
            rows[2 * s + blk] = jnp.where(rg == 0, x[0:1], x[7:8])

    @pl.when(rim)
    def _():
        lat = i + 2 * rg - 1
        spot = ((1 - rg) * NT + t) * 4 + ch * 2

        def send_f(k):
            s = around(t, k // 4, NT)
            send(rows.at[pl.ds(2 * s, 2)], lr.at[pl.ds(spot, 2)], 6 + rg, (s, lat, k % 4))

        loop(0, 4 * NT, send_f)

    def send_e(k):
        s = around(t, k // 2, NT)
        e = k % 2
        send(inc.at[2 * s + 1 - e], woth.at[t * 2 + rg], 5, (s, i, 2 - 2 * ch + e))

    loop(0, 2 * NT, send_e)

    def send_d(k):
        s = around(t, k // 2, NT)
        lon = ch * 2 + around(rg, k, 2)
        send(inc.at[pl.ds(2 * s, 2)], wown.at[pl.ds((t * 2 + rg) * 2, 2)], 4, (s, i, lon))

    loop(1, 2 * NT, send_d)

    wown[(t * 2 + rg) * 2] = inc[2 * t]
    wown[(t * 2 + rg) * 2 + 1] = inc[2 * t + 1]

    arrived(wown.at[pl.ds(0, 2 * (2 * NT - 1))], 4)
    arrived(woth, 5)

    @pl.when(i > 0)
    def _():
        arrived(lr.at[pl.ds(0, 4 * NT)], 7)

    @pl.when(i < NL - 1)
    def _():
        arrived(lr.at[pl.ds(4 * NT, 4 * NT)], 6)

    even = rg == 0
    w = wown[...].reshape(2 * NT, 2, 8, COLS)
    w0, w1 = w[:, 0].reshape(16 * NT, COLS), w[:, 1].reshape(16 * NT, COLS)
    lane = lax.broadcasted_iota(jnp.int32, (16 * NT, COLS), 1)
    near = jnp.where(even, 0, COLS - 1)
    far = COLS - 1 - near
    wbuf[:inner, :COLS] = jnp.where(even, w0, w1)
    wbuf[:inner, COLS:] = jnp.where(
        lane == near,
        jnp.where(even, w1, w0),
        jnp.where(lane == far, woth[...].reshape(16 * NT, COLS), 0.0),
    )
    lane1 = lax.broadcasted_iota(jnp.int32, (1, COLS), 1)
    for k in range(2 * NT):
        before = lr[k * 4 + (j + 3) % 4]
        after = lr[k * 4 + (j + 1) % 4]
        wbuf[inner + k : inner + k + 1, :COLS] = lr[k * 4 + j]
        wbuf[inner + k : inner + k + 1, COLS:] = jnp.where(
            lane1 == COLS - 1, before, jnp.where(lane1 == 0, after, 0.0)
        )

    r_both = rtb[...]
    r_high, r_low = r_both[:KR], r_both[KR:]
    w_high, w_low = halves(wbuf[...].T)
    both = nn(jnp.concatenate([w_high, w_low], axis=0), r_high)
    mixed = both[:256] + both[256:] + nn(w_high, r_low)
    cols = ctb[...]
    seen = jnp.sum(mixed * cols, axis=0, keepdims=True)
    departure = weight * (seen - target)
    d_high, d_low = halves(cols * departure)
    both = nt(r_both, d_high)
    g = both[:KR] + both[KR:] + nt(r_high, d_low)
    for k in range(2 * NT):
        gb[2 * k] = g[8 * k : 8 * k + 8, :COLS]
        gb[2 * k + 1] = g[8 * k : 8 * k + 8, COLS:]
    for k in range(2 * NT):
        grow[2 * k] = g[inner + k : inner + k + 1, :COLS]
        grow[2 * k + 1] = g[inner + k : inner + k + 1, COLS:]

    def send_rim(pos):
        def go(k):
            l = around(t, k // 2, NT)
            send(
                grow.at[pl.ds((pos * NT + l) * 2, 2)],
                glr.at[pl.ds((t * 4 + j) * 2, 2)],
                10 + pos,
                (l, i - 1 + 2 * pos, (k % 2) * 2 + 1 - pos),
            )

        loop(0, 2 * NT, go)

    @pl.when(i > 0)
    def _():
        send_rim(0)

    @pl.when(i < NL - 1)
    def _():
        send_rim(1)

    def send_h(k):
        l = around(t, k // 2, NT)
        half = k % 2
        send(
            gb.at[(l * 2 + half) * 2 + 1], goth.at[t * 2 + rg], 9, (l, i, 2 - 2 * ch + half)
        )

    loop(0, 2 * NT, send_h)

    def send_g(k):
        l = around(t, k // 2, NT)
        half = around(rg, k, 2)
        send(
            gb.at[pl.ds((l * 2 + half) * 2, 2)],
            gown.at[pl.ds((t * 2 + rg) * 2, 2)],
            8,
            (l, i, ch * 2 + half),
        )

    loop(1, 2 * NT, send_g)

    gown[(t * 2 + rg) * 2] = gb[(t * 2 + rg) * 2]
    gown[(t * 2 + rg) * 2 + 1] = gb[(t * 2 + rg) * 2 + 1]
    arrived(gown.at[pl.ds(0, 2 * (2 * NT - 1))], 8)
    arrived(goth, 9)

    @pl.when(jnp.logical_and(rim, rg == 1))
    def _():
        arrived(glr, 10)

    @pl.when(jnp.logical_and(rim, rg == 0))
    def _():
        arrived(glr, 11)

    lane8 = lax.broadcasted_iota(jnp.int32, (8, COLS), 1)
    row8 = lax.broadcasted_iota(jnp.int32, (8, COLS), 0)
    first, last = lane8 == 0, lane8 == COLS - 1
    mine = row8 == jnp.where(even, 0, 7)
    other = 2 - 2 * ch
    acc0 = acc1 = None
    for s in range(NT):
        def rim_of(b, part, s=s):
            return jnp.broadcast_to(glr[(s * 4 + b) * 2 + part], (8, COLS))

        d0 = gown[s * 4] + jnp.where(last, gown[s * 4 + 3], 0.0)
        d0 = d0 + jnp.where(first, goth[s * 2 + 1], 0.0)
        e0 = rim_of(ch * 2, 0) + jnp.where(last, rim_of(ch * 2 + 1, 1), 0.0)
        e0 = e0 + jnp.where(first, rim_of(other + 1, 1), 0.0)
        d0 = d0 + jnp.where(mine, e0, 0.0)
        d1 = gown[s * 4 + 2] + jnp.where(first, gown[s * 4 + 1], 0.0)
        d1 = d1 + jnp.where(last, goth[s * 2], 0.0)
        e1 = rim_of(ch * 2 + 1, 0) + jnp.where(first, rim_of(ch * 2, 1), 0.0)
        e1 = e1 + jnp.where(last, rim_of(other, 1), 0.0)
        d1 = d1 + jnp.where(mine, e1, 0.0)
        p0, p1 = pbuf[2 * s] * d0[None], pbuf[2 * s + 1] * d1[None]
        acc0, acc1 = (p0, p1) if s == 0 else (acc0 + p0, acc1 + p1)
    grad = jnp.concatenate([acc0.reshape(m8, COLS), acc1.reshape(m8, COLS)], axis=1)
    both = nn(jnp.concatenate(halves(grad), axis=0), lon_m)
    h = both[:m8] + both[m8:]
    for b in range(4):
        hbuf[NL * b : NL * b + NL] = h[:, b * COLS : (b + 1) * COLS].reshape(NL, 8, COLS)

    for spot in everywhere:
        lat, lon = place_at(spot)
        send(hbuf.at[lon * NL + lat], b2.at[ch * 2 * NL + 2 * i + rg], 12, (t, lat, lon))

    b2[ch * 2 * NL + 2 * i + rg] = hbuf[j * NL + i]
    arrived(b2.at[pl.ds(0, 4 * NL - 1)], 12)
    y = (b2[: 2 * NL] + b2[2 * NL :]).reshape(NL * ROWS, COLS)
    high, low = halves(y)
    both = nn(lat_t, jnp.concatenate([high, low], axis=1))
    adb[...] = (both[:, :COLS] + both[:, COLS:]).reshape(NL, ROWS, COLS)

    for step in lat_steps:
        to = lat_at(step)
        send(adb.at[to], gat.at[i, t], 13, (t, to, j))

    gat[i, t] = adb[i]

    chunks = 4 if NL % 4 == 0 else NL
    size = NL // chunks
    half = chunks // 2
    chips = NT // 2
    core = lax.rem(t, jnp.int32(2))
    sibling = t + 1 - 2 * core
    right, left = around(t, 2, NT), around(t, NT - 2, NT)
    across = around(t, NT // 2, NT)

    def chunk(c, owner):
        return gat.at[pl.ds(c * size, size), owner]

    def pass_on(ref, n, to):
        pltpu.make_async_remote_copy(
            src_ref=ref,
            dst_ref=ref,
            send_sem=ssem.at[14],
            recv_sem=hsem.at[n],
            device_id=(to, i, j),
            device_id_type=MESH,
        ).start()

    def landed(c, n):
        pltpu.make_async_copy(chunk(c, t), chunk(c, t), hsem.at[n]).wait()

    outward = []

    def to_out(owner):
        n = len(outward)
        outward.append(pltpu.make_async_copy(gat.at[:, owner], out.at[:, owner], lsem.at[n]))
        outward[-1].start()

    from_left, from_right, from_far, from_sibling = 0, chunks, 2 * chunks, 3 * chunks
    rightward = list(range(chunks))
    leftward = rightward[half:] + rightward[:half]
    arrived(gat.at[pl.ds(0, NL - 1), t], 13)
    if chips > 1:
        for c, d in zip(rightward, leftward):
            pass_on(chunk(c, t), from_left + c, right)
            pass_on(chunk(d, t), from_right + d, left)
    pass_on(gat.at[:, t], from_sibling, sibling)
    to_out(t)
    if chips > 1:
        for c, d in zip(rightward, leftward):
            landed(c, from_left + c)
            if c < half:
                pass_on(chunk(c, left), from_far + c, right)
            pass_on(chunk(c, left), from_sibling, sibling)
            landed(d, from_right + d)
            if d >= half:
                pass_on(chunk(d, right), from_far + d, left)
            pass_on(chunk(d, right), from_sibling, sibling)
        to_out(left)
        to_out(right)
        for n in range(chunks):
            c = n // 2 + (n % 2) * half if chunks % 2 == 0 else n
            landed(c, from_far + c)
            pass_on(chunk(c, across), from_sibling, sibling)
        to_out(across)
    everything = gat.at[:, pl.ds(0, chips)]
    pltpu.make_async_copy(everything, everything, hsem.at[from_sibling]).wait()
    for chip in range(chips):
        to_out(2 * chip + 1 - core)

    sent(abuf.at[pl.ds(0, NL - 1)], 0)
    sent(obuf.at[pl.ds(0, NT - 1)], 1)
    sent(pbuf.at[pl.ds(0, 2 * NT - 1)], 2)
    sent(bbuf.at[pl.ds(0, 4 * NL - 1)], 3)
    sent(wown.at[pl.ds(0, 2 * (2 * NT - 1))], 4)
    sent(woth, 5)

    @pl.when(jnp.logical_and(rim, rg == 0))
    def _():
        sent(glr, 6)

    @pl.when(jnp.logical_and(rim, rg == 1))
    def _():
        sent(glr, 7)

    sent(gown.at[pl.ds(0, 2 * (2 * NT - 1))], 8)
    sent(goth, 9)

    @pl.when(i > 0)
    def _():
        sent(lr.at[pl.ds(0, 4 * NT)], 10)

    @pl.when(i < NL - 1)
    def _():
        sent(lr.at[pl.ds(0, 4 * NT)], 11)

    sent(b2.at[pl.ds(0, 4 * NL - 1)], 12)
    sent(gat.at[pl.ds(0, NL - 1), t], 13)
    sent(gat.at[:, pl.ds(0, NT - 1)], 14)
    for copy in outward:
        copy.wait()


def per_device(NT, NL, control, pert, latf, lonf, ilat, ilon, cell, count, value, weight):
    hbm = pl.BlockSpec(memory_space=pltpu.HBM)
    V = pltpu.VMEM
    tile = (8, COLS)
    cap = cell.shape[-1]
    scratch = [
        V((ROWS + 2, FINE_ROWS), F32),
        V((COLS + 2, FINE_COLS), F32),
        V((NT, 1, cap), jnp.int32),
        V((1, NT), jnp.int32),
        V((NT, 1, cap), F32),
        V((NT, 1, cap), F32),
        V((NT, *tile), F32),
        V((NL, ROWS, COLS), F32),
        V((NL, NT, ROWS, COLS), BF16),
        V((NL * ROWS, NL * ROWS), BF16),
        V((256, 512), BF16),
        V((NL, ROWS, COLS), F32),
        V((NT, *tile), F32),
        V((2 * NT, NL, *tile), F32),
        V((2 * NT, NL, *tile), F32),
        V((2 * NL, *tile), F32),
        V((4 * NL, *tile), F32),
        V((2 * NT, *tile), F32),
        V((2 * NT, 1, COLS), F32),
        V((4 * NT, *tile), F32),
        V((2 * NT, *tile), F32),
        V((8 * NT, 1, COLS), F32),
        V((KR, 256), F32),
        V((2 * KR, NT * 64), BF16),
        V((256, NT * 64), F32),
        V((4 * NT, *tile), F32),
        V((4 * NT, 1, COLS), F32),
        V((4 * NT, *tile), F32),
        V((2 * NT, *tile), F32),
        V((8 * NT, 1, COLS), F32),
        V((4 * NL, *tile), F32),
        V((4 * NL, *tile), F32),
        V((NL, ROWS, COLS), F32),
        V((NL, NT, ROWS, COLS), F32),
        pltpu.SemaphoreType.DMA((10,)),
        pltpu.SemaphoreType.DMA((15,)),
        pltpu.SemaphoreType.DMA((15,)),
        pltpu.SemaphoreType.DMA((13,)),
    ]
    adjoint = pl.pallas_call(
        functools.partial(kernel, NT, NL),
        name="gradient",
        out_shape=jax.ShapeDtypeStruct(control.shape, F32),
        in_specs=[hbm] * 10,
        out_specs=hbm,
        scratch_shapes=scratch,
        compiler_params=pltpu.CompilerParams(
            has_side_effects=True, collective_id=0, vmem_limit_bytes=63 * 1024 * 1024
        ),
    )(
        control,
        pert[0],
        latf,
        lonf,
        ilat.T,
        ilon.T,
        cell.reshape(NT, 1, cap),
        count.reshape(1, NT),
        value.reshape(NT, 1, cap),
        weight.reshape(NT, 1, cap),
    )
    return control + adjoint


def solution(mesh):
    placed = (
        P(None, None, "lat", "lon"),
        P("tm", None, None, "lat", "lon"),
        P(),
        P(),
        P("lat", None),
        P("lon", None),
        P("tm", None, "lat", "lon", None),
        P("tm", None, "lat", "lon"),
        P("tm", None, "lat", "lon", None),
        P("tm", None, "lat", "lon", None),
    )
    return jax.shard_map(
        functools.partial(per_device, mesh.shape["tm"], mesh.shape["lat"]),
        mesh=mesh,
        in_specs=placed,
        out_specs=P(None, None, "lat", "lon"),
        check_vma=False,
    )
```
